256 devices in a mesh: tm: 32 (over z, y), sx: 4 (over x), sy: 2 (over core).
Axes of the slice: x: 4, y: 4, z: 8, core: 2. Of those that a mesh axis runs over, the one named last changes fastest.
Arguments:
- thickness_guess: float32 [32, 1024, 256], P('tm', 'sx', 'sy'), may hold values from 0.5 to 1.5
- thickness_start: float32 [1024, 256], P('sx', 'sy'), may hold values from 0.5 to 1.5
- bed: float32 [1024, 256], P('sx', 'sy'), may hold values from -1.8 to 1.8
- rate_factor: float32 [1024, 256], P('sx', 'sy'), may hold values from 0.05 to 0.5
- mass_balance: float32 [32, 1024, 256], P('tm', 'sx', 'sy'), may hold values from -1.2 to 1.2
- cell_flags: int32 [1024, 256], P('sx', 'sy'), may hold values from 0 to 2, as said below
Outputs:
- thickness: float32 [32, 1024, 256], P('tm', 'sx', 'sy')
The draws below stay inside these ranges and needn't reach their ends.
Inputs may be any that keep to these rules, and one draw needn't show every extreme that they name: `cell_flags`: 0 marks ice-free cells outside the glacier, 1 ice on bedrock, 2 ice on soft sediment.
All inputs are finite; a program needn't handle non-finite values.
Results may differ from the reference program's by a relative error of at most 0.00015.
Values sent between devices are 32-bit elements; how exact they have to be, the bound alone decides.
A program may use at most 64 MiB of HBM per device.

```python
import math
import jax
import jax.numpy as jnp
from jax import lax

NEWTON = 2
SWEEPS = 8
LEVELS = 32
NX = 1024
NY = 256


def ellipse_union(key, members, narrow, broad):
    keys = jax.random.split(key, 4)
    row_grid = lax.broadcasted_iota(jnp.int32, (NX, NY), 0)
    col_grid = lax.broadcasted_iota(jnp.int32, (NX, NY), 1)
    centre_row = jax.random.randint(keys[0], (members,), 0, NX)
    centre_col = jax.random.randint(keys[1], (members,), 0, NY)
    radius_row = jax.random.randint(keys[2], (members,), max(NX // narrow, 1), max(NX // broad, 2))
    radius_col = jax.random.randint(keys[3], (members,), max(NY // narrow, 1), max(NY // broad, 2))
    covered = jnp.zeros((NX, NY), jnp.int32)
    for member in range(members):
        reach_row = row_grid - centre_row[member]
        reach_col = col_grid - centre_col[member]
        measure = reach_row * reach_row * 256 // (radius_row[member] * radius_row[member]) + reach_col * reach_col * 256 // (radius_col[member] * radius_col[member])
        covered = jnp.maximum(covered, (measure <= 256).astype(jnp.int32))
    return covered


def draw_cell_flags(key, part):
    base = jax.random.fold_in(key, 11)
    glacier = ellipse_union(jax.random.fold_in(base, 1), 12, 8, 4)
    sediment = ellipse_union(jax.random.fold_in(base, 2), 8, 16, 8)
    return (glacier * (1 + sediment)).astype(jnp.int32)


def block_scale(rng, shape, cuts, least, largest):
    def one(dim, shards_of):
        draws = jax.random.uniform(jax.random.fold_in(jax.random.fold_in(rng, 6), dim), (shards_of,), jnp.float32, least / len(cuts), largest / len(cuts))
        return jnp.repeat(jnp.exp(draws), shape[dim] // shards_of).reshape((-1,) + (1,) * (len(shape) - dim - 1))

    loudness = one(*cuts[0])
    for cut in cuts[1:]:
        loudness = loudness * one(*cut)
    return loudness


def gaussian(key, extent, width, limit, cuts=(), dtype=jnp.bfloat16):
    array = jax.random.normal(key, extent, jnp.float32) * width
    if len(cuts) > 0:
        array = block_scale(key, extent, cuts, -0.22, 0.18) * array
    return jnp.clip(array, min=-limit, max=limit).astype(dtype)


def setup_inputs(seed: int = 0) -> dict:
    splits = jax.random.split(jax.random.key(seed), 7)
    return {
        "thickness_guess": jnp.clip(0.5 + 1.0 * jax.random.uniform(splits[0], (LEVELS, NX, NY), jnp.float32) ** block_scale(splits[0], (LEVELS, NX, NY), ((0, 32), (1, 4), (2, 2)), -0.2, 0.2), 0.5, 1.5),
        "thickness_start": jnp.clip(0.5 + 1.0 * jax.random.uniform(splits[1], (NX, NY), jnp.float32) ** block_scale(splits[1], (NX, NY), ((0, 4), (1, 2)), -0.2, 0.2), 0.5, 1.5),
        "bed": gaussian(splits[2], (NX, NY), 0.3, 1.8, ((0, 4), (1, 2)), jnp.float32),
        "rate_factor": jnp.clip(jnp.exp(math.log(0.5) - 2.3025851 * jax.random.uniform(splits[3], (NX, NY), jnp.float32) ** block_scale(splits[3], (NX, NY), ((0, 4), (1, 2)), -0.2, 0.2)), 0.05, 0.5),
        "mass_balance": gaussian(splits[4], (LEVELS, NX, NY), 0.2, 1.2, ((0, 32), (1, 4), (2, 2)), jnp.float32),
        "cell_flags": draw_cell_flags(jax.random.fold_in(splits[6], 71), 0),
    }


circulant_weight = 0.25
time_step = 1.0


def cell_diffusivity(thickness, rate_factor, cell_flags):
    inside = (cell_flags != 0).astype(jnp.float32)
    boost = 1.0 + (cell_flags == 2).astype(jnp.float32)
    return inside * boost * rate_factor * thickness * thickness * jnp.abs(thickness)


def face_weights(padded):
    centre = padded[1:-1, 1:-1]
    return (0.5 * (centre + padded[2:, 1:-1]), 0.5 * (centre + padded[:-2, 1:-1]),
            0.5 * (centre + padded[1:-1, 2:]), 0.5 * (centre + padded[1:-1, :-2]))


def neighbour_sum(weights, padded):
    return (weights[0] * padded[2:, 1:-1] + weights[1] * padded[:-2, 1:-1]
            + weights[2] * padded[1:-1, 2:] + weights[3] * padded[1:-1, :-2])


def reference(thickness_guess, thickness_start, bed, rate_factor, mass_balance, cell_flags):
    levels = thickness_guess.shape[0]
    inside = (cell_flags != 0).astype(jnp.float32)
    ratio_root = circulant_weight ** (1.0 / levels)
    level_range = jnp.arange(levels).astype(jnp.float32)
    weight_up = ratio_root ** level_range
    mode_angle = (2.0 * math.pi / levels) * level_range
    shift_real = (1.0 - ratio_root * jnp.cos(mode_angle)) / time_step
    shift_imag = ratio_root * jnp.sin(mode_angle) / time_step
    thickness = thickness_guess
    for newton_step in range(NEWTON):
        prior_level = jnp.concatenate([thickness_start[None], thickness[:-1]], 0)

        def residual_of(operands):
            level_thickness, level_prior, level_balance = operands
            diffuse = cell_diffusivity(level_thickness, rate_factor, cell_flags)
            weights = face_weights(jnp.pad(diffuse, 1))
            face_total = weights[0] + weights[1] + weights[2] + weights[3]
            surface = level_thickness + bed
            change = ((level_thickness - level_prior) / time_step + face_total * surface
                      - neighbour_sum(weights, jnp.pad(surface, 1)) - level_balance)
            return inside * change, diffuse

        residual, diffuse = lax.map(residual_of, (thickness, prior_level, mass_balance))
        mean_diff = jnp.sum(diffuse, axis=0) / levels
        weights = face_weights(jnp.pad(mean_diff, 1))
        face_total = weights[0] + weights[1] + weights[2] + weights[3]
        spectrum = jnp.fft.fft(residual * weight_up[:, None, None], axis=0)
        spectrum_real = jnp.real(spectrum)
        spectrum_imag = jnp.imag(spectrum)

        def solve_mode(operands):
            source_real, source_imag, one_real, one_imag = operands
            denom_real = one_real + face_total
            denom_norm = denom_real * denom_real + one_imag * one_imag
            inverse_real = inside * denom_real / denom_norm
            inverse_imag = -inside * one_imag / denom_norm
            value_real = source_real * inverse_real - source_imag * inverse_imag
            value_imag = source_real * inverse_imag + source_imag * inverse_real
            for sweep_index in range(SWEEPS - 1):
                numer_real = source_real + neighbour_sum(weights, jnp.pad(value_real, 1))
                numer_imag = source_imag + neighbour_sum(weights, jnp.pad(value_imag, 1))
                value_real = numer_real * inverse_real - numer_imag * inverse_imag
                value_imag = numer_real * inverse_imag + numer_imag * inverse_real
            return value_real, value_imag

        solution_real, solution_imag = lax.map(solve_mode, (spectrum_real, spectrum_imag, shift_real, shift_imag))
        update = jnp.real(jnp.fft.ifft(solution_real, axis=0)) - jnp.imag(jnp.fft.ifft(solution_imag, axis=0))
        thickness = thickness - update / weight_up[:, None, None]
    return thickness
```

```python
import functools
import math

import jax
import jax.numpy as jnp
from jax import lax
from jax.experimental import pallas as pl
from jax.experimental.pallas import tpu as pltpu
from jax.sharding import PartitionSpec as P

NEWTON = 2
SWEEPS = 8
RING_Y = 4
ROWS = 8
LANES = 128
WIDE = 2 * LANES
EXT = 3 * ROWS

circulant_weight = 0.25
time_step = 1.0
MESH = pl.DeviceIdType.MESH


def forward_modes(u, half, levels, odd):
    mid = half // 2
    out = []
    if not odd:
        even = [u[l] + u[half - l] for l in range(1, mid)]
        diff = [u[l] - u[half - l] for l in range(1, mid)]
        plus, minus = u[0] + u[mid], u[0] - u[mid]
        for m in range(mid):
            real = plus if m % 2 == 0 else minus
            for l in range(1, mid):
                real = real + even[l - 1] * math.cos(2 * math.pi * l * m / half)
            if m == 0:
                imag = plus if mid % 2 == 0 else minus
                for l in range(1, mid):
                    imag = imag + even[l - 1] * (-1.0) ** l
            else:
                imag = None
                for l in range(1, mid):
                    term = diff[l - 1] * -math.sin(2 * math.pi * l * m / half)
                    imag = term if imag is None else imag + term
            out.append((real, imag))
    else:
        diff = [u[l] - u[half - l] for l in range(1, mid)]
        both = [u[l] + u[half - l] for l in range(1, mid)]
        for m in range(mid):
            k = 2 * m + 1
            real = u[0]
            imag = u[mid] * -math.sin(math.pi * k / 2)
            for l in range(1, mid):
                real = real + diff[l - 1] * math.cos(2 * math.pi * l * k / levels)
                imag = imag + both[l - 1] * -math.sin(2 * math.pi * l * k / levels)
            out.append((real, imag))
    return out


def inverse_modes(v, half, levels, odd):
    mid = half // 2
    out = [None] * half
    scale = 2.0 / levels
    for l in range(mid + 1):
        if not odd:
            cosine = v[0] * (1.0 / levels) + v[1] * ((-1.0) ** l / levels)
            sine = None
            for m in range(1, mid):
                cosine = cosine + v[2 * m] * (scale * math.cos(2 * math.pi * l * m / half))
                if l not in (0, mid):
                    term = v[2 * m + 1] * (scale * math.sin(2 * math.pi * l * m / half))
                    sine = term if sine is None else sine + term
            low = cosine if sine is None else cosine - sine
            high = cosine if sine is None else cosine + sine
        else:
            cosine = sine = None
            for m in range(mid):
                k = 2 * m + 1
                term = v[2 * m] * (scale * math.cos(2 * math.pi * l * k / levels))
                cosine = term if cosine is None else cosine + term
                if l > 0:
                    term = v[2 * m + 1] * (scale * math.sin(2 * math.pi * l * k / levels))
                    sine = term if sine is None else sine + term
            low = cosine if sine is None else cosine - sine
            high = -cosine if sine is None else -cosine - sine
        out[l] = low
        if 0 < l < half:
            out[half - l] = high if l != mid else low
    return out


def kernel(
    levels, stripes,
    guess_ref, start_ref, bed_ref, rate_ref, balance_ref, flags_ref,
    out_ref,
    guess, balance, bed_in, rate_in, flags_in,
    own, edge, mass, stat_send, stat, row_send, rows,
    dsend, dext, resid, ysend, yext, coef, weight, modes, parts, dummy,
    load_sem, gsend, grecv, bsend, brecv, ssend, srecv, osend, orecv,
    esend, erecv, hsend, hrecv, dsem_s, dsem_r, ysem_s, ysem_r, psem_s, psem_r,
):
    half = levels // 2
    slots = half // 2
    ring_z = levels // RING_Y
    tiles = stripes * levels
    root = circulant_weight ** (1.0 / levels)

    level = lax.axis_index("tm")
    sx = lax.axis_index("sx")
    core = lax.axis_index("sy")
    other = 1 - core
    mine = pl.ds(pl.multiple_of(core * LANES, LANES), LANES)
    theirs = pl.ds(pl.multiple_of(other * LANES, LANES), LANES)

    def tile_of(stripe, tm):
        z, y = tm // RING_Y, tm % RING_Y
        place = z * RING_Y + jnp.where(z % 2 == 0, y, RING_Y - 1 - y)
        return jnp.where(stripe % 2 == 0, place, levels - 1 - place)

    def owner_of(stripe, tile):
        place = jnp.where(stripe % 2 == 0, tile, levels - 1 - tile)
        z, y = place // RING_Y, place % RING_Y
        return z * RING_Y + jnp.where(z % 2 == 0, y, RING_Y - 1 - y)

    tile = tile_of(sx, level)
    strip = sx * levels + tile
    above = (strip + tiles - 1) % tiles
    below = (strip + 1) % tiles
    above_sx, below_sx = above // levels, below // levels
    above_tm = owner_of(above_sx, above % levels)
    below_tm = owner_of(below_sx, below % levels)
    has_above = strip > 0
    has_below = strip < tiles - 1

    def peer(step):
        iz, iy = step // RING_Y, step % RING_Y
        sign_z = 1 - 2 * (iz % 2)
        sign_y = 1 - 2 * (iy % 2)
        z = (level // RING_Y + ring_z // 2 + sign_z * ((iz + 1) // 2) + ring_z) % ring_z
        y = (level % RING_Y + RING_Y // 2 + sign_y * ((iy + 1) // 2) + RING_Y) % RING_Y
        return z * RING_Y + y

    def send(src, dst, ssem, rsem, device):
        pltpu.make_async_remote_copy(
            src_ref=src, dst_ref=dst, send_sem=ssem, recv_sem=rsem,
            device_id=device, device_id_type=MESH,
        ).start()

    def wait(sem, count):
        view = dummy.at[pl.ds(0, count)]
        pltpu.make_async_copy(view, view, sem).wait()

    def around(src, place, ssem, rsem):
        send(src, place(1), ssem, rsem, (level, sx, other))
        for to in range(2):
            send(src, place(2), ssem, rsem, (above_tm, above_sx, to))
            send(src, place(0), ssem, rsem, (below_tm, below_sx, to))

    barrier = pltpu.get_barrier_semaphore()

    def greet(step, carry):
        pl.semaphore_signal(barrier, inc=1, device_id=(peer(step), sx, core), device_id_type=MESH)
        return carry

    lax.fori_loop(0, levels - 1, greet, 0)
    pl.semaphore_signal(barrier, inc=1, device_id=(level, sx, other), device_id_type=MESH)
    for to in range(2):
        pl.semaphore_signal(barrier, inc=1, device_id=(above_tm, above_sx, to), device_id_type=MESH)
        pl.semaphore_signal(barrier, inc=1, device_id=(below_tm, below_sx, to), device_id_type=MESH)

    here = pl.ds(pl.multiple_of(tile * ROWS, ROWS), ROWS)
    loads = [
        pltpu.make_async_copy(guess_ref.at[0], guess, load_sem.at[0]),
        pltpu.make_async_copy(balance_ref.at[0], balance, load_sem.at[1]),
        pltpu.make_async_copy(bed_ref.at[here], bed_in, load_sem.at[2]),
        pltpu.make_async_copy(rate_ref.at[here], rate_in, load_sem.at[3]),
        pltpu.make_async_copy(flags_ref.at[here], flags_in, load_sem.at[4]),
        pltpu.make_async_copy(start_ref.at[here], own.at[0, :, mine], load_sem.at[5]),
    ]
    for load in loads:
        load.start()
    for load in loads:
        load.wait()

    inside_own = (flags_in[...] != 0).astype(jnp.float32)
    boost = 1.0 + (flags_in[...] == 2).astype(jnp.float32)
    cst_own = inside_own * boost * rate_in[...]
    bed_own = bed_in[...]
    for i, value in enumerate((cst_own, bed_own, inside_own)):
        stat_send[i] = value
        stat[i, ROWS : 2 * ROWS, mine] = value

    pl.semaphore_wait(barrier, levels - 1 + 5)

    def scatter(src, dst, ssem, rsem):
        def step(i, carry):
            to = peer(i)
            rows_to = pl.ds(pl.multiple_of(tile_of(sx, to) * ROWS, ROWS), ROWS)
            send(src.at[rows_to], dst, ssem, rsem, (to, sx, core))
            return carry

        lax.fori_loop(0, levels - 1, step, 0)

    scatter(guess, own.at[1 + level, :, mine], gsend, grecv)
    scatter(balance, mass.at[level], bsend, brecv)
    around(
        stat_send, lambda p: stat.at[:, pl.ds(p * ROWS, ROWS), mine], ssend, srecv
    )
    own[1 + level, :, mine] = guess[here]
    mass[level] = balance[here]

    wait(grecv, levels - 1)
    all_levels = pl.ds(1, levels)
    send(
        own.at[all_levels, :, mine], own.at[all_levels, :, mine], hsend, hrecv,
        (level, sx, other),
    )
    for l in range(levels):
        row_send[0, l : l + 1] = own[1 + l, 0:1, mine]
        row_send[1, l : l + 1] = own[1 + l, ROWS - 1 : ROWS, mine]
    send(row_send.at[0], rows.at[1], esend, erecv, (above_tm, above_sx, core))
    send(row_send.at[1], rows.at[0], esend, erecv, (below_tm, below_sx, core))

    row8 = lax.broadcasted_iota(jnp.int32, (ROWS, LANES), 0)
    lane = lax.broadcasted_iota(jnp.int32, (ROWS, LANES), 1)
    first_row, last_row = row8 == 0, row8 == ROWS - 1
    first_lane, last_lane = lane == 0, lane == LANES - 1
    edge_valid = (last_row & has_above) | (first_row & has_below)

    def neighbours(x, x_other, x_edge):
        right = pltpu.roll(jnp.where(first_lane, jnp.where(core == 0, x_other, 0.0), x), LANES - 1, 1)
        left = pltpu.roll(jnp.where(last_lane, jnp.where(core == 1, x_other, 0.0), x), 1, 1)
        down = pltpu.roll(jnp.where(first_row, x_edge, x), ROWS - 1, 0)
        up = pltpu.roll(jnp.where(last_row, x_edge, x), 1, 0)
        return right, left, down, up

    wait(srecv, 3 * 5)
    wait(erecv, 2 * (levels // ROWS))
    for l in range(levels):
        edge[l] = jnp.where(last_row, rows[0, l : l + 1], rows[1, l : l + 1])

    cst_other = stat[0, ROWS : 2 * ROWS, theirs]
    bed_other = stat[1, ROWS : 2 * ROWS, theirs]
    cst_edge = jnp.where(
        edge_valid, jnp.where(last_row, stat[0, 0:ROWS, mine], stat[0, 2 * ROWS :, mine]), 0.0
    )
    bed_edge = jnp.where(last_row, stat[1, 0:ROWS, mine], stat[1, 2 * ROWS :, mine])

    row_wide = lax.broadcasted_iota(jnp.int32, (EXT, WIDE), 0)
    col_wide = lax.broadcasted_iota(jnp.int32, (EXT, WIDE), 1)
    valid_wide = (
        ((row_wide >= ROWS) | has_above) & ((row_wide < 2 * ROWS) | has_below)
    )

    wait(hrecv, levels)

    def diffusivity(scale, h):
        return scale * h * h * jnp.abs(h)

    def newton(n, carry):
        def add_up(l, sums):
            return (
                sums[0] + diffusivity(cst_own, own[1 + l, :, mine]),
                sums[1] + diffusivity(cst_other, own[1 + l, :, theirs]),
                sums[2] + diffusivity(cst_edge, edge[l]),
            )

        zero = jnp.zeros((ROWS, LANES), jnp.float32)
        sums = lax.fori_loop(0, levels, add_up, (zero, zero, zero))
        mean, mean_other, mean_edge = (s * (1.0 / levels) for s in sums)
        total = 0.5 * (4.0 * mean + sum(neighbours(mean, mean_other, mean_edge)))
        for i, value in enumerate((mean, total)):
            dsend[n, i] = value
            dext[n, i, ROWS : 2 * ROWS, mine] = value
        around(
            dsend.at[n],
            lambda p: dext.at[n, :, pl.ds(p * ROWS, ROWS), mine],
            dsem_s.at[n], dsem_r.at[n],
        )

        @pl.when(n == 0)
        def _():
            wait(brecv, levels - 1)

        def residual(l, lift):
            h, h_other, h_edge = own[1 + l, :, mine], own[1 + l, :, theirs], edge[l]
            d = diffusivity(cst_own, h)
            s = h + bed_own
            d_near = neighbours(
                d, diffusivity(cst_other, h_other), diffusivity(cst_edge, h_edge)
            )
            s_near = neighbours(
                s, h_other + bed_other, jnp.where(edge_valid, h_edge + bed_edge, 0.0)
            )
            flux = sum((d + dn) * (s - sn) for dn, sn in zip(d_near, s_near))
            change = (h - own[l, :, mine]) / time_step + 0.5 * flux - mass[l]
            resid[l] = inside_own * change * lift
            return lift * root

        lax.fori_loop(0, levels, residual, jnp.ones((ROWS, LANES), jnp.float32))

        low = [resid[l] for l in range(half)]
        high = [resid[l + half] for l in range(half)]
        evens = forward_modes([a + b for a, b in zip(low, high)], half, levels, False)
        odds = forward_modes([a - b for a, b in zip(low, high)], half, levels, True)
        for slot in range(slots):
            for i in range(2):
                ysend[n, 0, 2 * slot + i] = evens[slot][i]
                ysend[n, 1, 2 * slot + i] = odds[slot][i]
                yext[n, 2 * slot + i, ROWS : 2 * ROWS, mine] = jnp.where(
                    core == 0, evens[slot][i], odds[slot][i]
                )
            pair = pl.ds(2 * slot, 2)

            def place(p):
                return yext.at[n, pair, pl.ds(p * ROWS, ROWS), mine]

            s_sem, r_sem = ysem_s.at[n], ysem_r.at[n, slot]
            send(ysend.at[n, other, pair], place(1), s_sem, r_sem, (level, sx, other))
            for to in range(2):
                send(ysend.at[n, to, pair], place(2), s_sem, r_sem, (above_tm, above_sx, to))
                send(ysend.at[n, to, pair], place(0), s_sem, r_sem, (below_tm, below_sx, to))

        wait(dsem_r.at[n], 2 * 5)
        mean_wide = jnp.where(valid_wide, dext[n, 0], 0.0)
        total_wide = dext[n, 1]
        inside_wide = jnp.where(valid_wide, stat[2], 0.0)
        weight[0] = jnp.where(
            col_wide == WIDE - 1, 0.0, 0.5 * (mean_wide + pltpu.roll(mean_wide, WIDE - 1, 1))
        )
        weight[1] = jnp.where(col_wide == 0, 0.0, 0.5 * (mean_wide + pltpu.roll(mean_wide, 1, 1)))
        weight[2] = 0.5 * (mean_wide + pltpu.roll(mean_wide, EXT - 1, 0))
        weight[3] = 0.5 * (mean_wide + pltpu.roll(mean_wide, 1, 0))
        for m in range(slots):
            def shift(k):
                angle = 2 * math.pi * k / levels
                return (
                    (1.0 - root * math.cos(angle)) / time_step,
                    root * math.sin(angle) / time_step,
                )

            even_real, even_imag = shift(2 * m)
            odd_real, odd_imag = shift(2 * m + 1)
            last_real = shift(half)[0] if m == 0 else even_real
            real = total_wide + jnp.where(core == 0, even_real, odd_real)
            real_2 = total_wide + jnp.where(core == 0, last_real, odd_real)
            imag = jnp.where(core == 0, 0.0 if m == 0 else even_imag, odd_imag)
            scaled = inside_wide / (real * real + imag * imag)
            coef[m, 0] = scaled * real
            coef[m, 1] = scaled * -imag
            coef[m, 2] = inside_wide * real_2 / (real_2 * real_2 + imag * imag)

        def solve(slot, carry):
            wait(ysem_r.at[n, slot], 2 * 5)
            source_real = yext[n, 2 * slot]
            source_imag = yext[n, 2 * slot + 1]
            a, b, c = coef[slot, 0], coef[slot, 1], coef[slot, 2]

            def apply(real, imag):
                return real * a - imag * b, real * b + imag * c

            def spread(v):
                return (
                    weight[0] * pltpu.roll(v, WIDE - 1, 1)
                    + weight[1] * pltpu.roll(v, 1, 1)
                    + weight[2] * pltpu.roll(v, EXT - 1, 0)
                    + weight[3] * pltpu.roll(v, 1, 0)
                )

            real, imag = apply(source_real, source_imag)
            for _ in range(SWEEPS - 1):
                real, imag = apply(source_real + spread(real), source_imag + spread(imag))
            for i, v in enumerate((real, imag)):
                for h in range(2):
                    cols = slice(h * LANES, (h + 1) * LANES)
                    modes[h, 2 * slot + i] = v[ROWS : 2 * ROWS, cols]
                    modes[2 + h, 2 * slot + i] = jnp.where(last_row, v[0:ROWS, cols], v[2 * ROWS :, cols])
            return carry

        lax.fori_loop(0, slots, solve, 0)

        for parity in range(2):
            @pl.when(core == parity)
            def _():
                def invert(p, carry):
                    values = inverse_modes(
                        [modes[p, f] for f in range(half)], half, levels, parity == 1
                    )
                    for l in range(half):
                        parts[n, parity, p, l] = values[l]
                    return carry

                lax.fori_loop(0, 4, invert, 0)

        send(
            parts.at[n, core], parts.at[n, core], psem_s.at[n], psem_r.at[n], (level, sx, other)
        )
        wait(psem_r.at[n], 4 * half)

        def update(l, drop):
            far = drop * (root ** -half)
            for h in range(2):
                cols = slice(h * LANES, (h + 1) * LANES)
                p, q = parts[n, 0, h, l], parts[n, 1, h, l]
                own[1 + l, :, cols] = own[1 + l, :, cols] - (p + q) * drop
                own[1 + half + l, :, cols] = own[1 + half + l, :, cols] - (p - q) * far
            p, q = parts[n, 0, 2 + core, l], parts[n, 1, 2 + core, l]
            edge[l] = edge[l] - (p + q) * drop
            edge[half + l] = edge[half + l] - (p - q) * far
            return drop * (1.0 / root)

        @pl.when(n == 0)
        def _():
            wait(hsend, levels)

        lax.fori_loop(0, half, update, jnp.ones((ROWS, LANES), jnp.float32))
        return carry

    lax.fori_loop(0, NEWTON, newton, 0)

    def give(i, carry):
        to = peer(i)
        send(own.at[1 + to, :, mine], out_ref.at[0, here], osend, orecv, (to, sx, core))
        return carry

    lax.fori_loop(0, levels - 1, give, 0)
    out_ref[0, here] = own[1 + level, :, mine]

    wait(gsend, levels - 1)
    wait(bsend, levels - 1)
    wait(ssend, 3 * 5)
    wait(esend, 2 * (levels // ROWS))
    for n in range(NEWTON):
        wait(dsem_s.at[n], 2 * 5)
        wait(ysem_s.at[n], 2 * 5 * slots)
        wait(psem_s.at[n], 4 * half)
    wait(osend, levels - 1)
    wait(orecv, levels - 1)


def solution(mesh):
    levels, stripes = mesh.shape["tm"], mesh.shape["sx"]
    half = levels // 2
    slots = half // 2
    tile = (ROWS, LANES)
    f32 = jnp.float32

    def vmem(*lead, last=tile, dtype=f32):
        return pltpu.VMEM((*lead, *last), dtype)

    dma = pltpu.SemaphoreType.DMA

    def body(guess, start, bed, rate, balance, flags):
        rows = guess.shape[1]
        return pl.pallas_call(
            functools.partial(kernel, levels, stripes),
            out_shape=jax.ShapeDtypeStruct(guess.shape, f32),
            in_specs=[pl.BlockSpec(memory_space=pl.ANY)] * 6,
            out_specs=pl.BlockSpec(memory_space=pltpu.VMEM),
            scratch_shapes=[
                vmem(last=(rows, LANES)), vmem(last=(rows, LANES)),
                vmem(), vmem(), vmem(dtype=jnp.int32),
                vmem(levels + 1, last=(ROWS, WIDE)), vmem(levels), vmem(levels),
                vmem(3), vmem(3, last=(EXT, WIDE)),
                vmem(2, last=(levels, LANES)), vmem(2, last=(levels, LANES)),
                vmem(NEWTON, 2), vmem(NEWTON, 2, last=(EXT, WIDE)),
                vmem(levels), vmem(NEWTON, 2, half),
                vmem(NEWTON, half, last=(EXT, WIDE)),
                vmem(slots, 3, last=(EXT, WIDE)), vmem(4, last=(EXT, WIDE)),
                vmem(4, half), vmem(NEWTON, 2, 4, half),
                vmem(max(2 * 5 * slots, 4 * half, levels)),
                dma((6,)), dma, dma, dma, dma, dma, dma, dma, dma,
                dma, dma, dma, dma, dma((NEWTON,)), dma((NEWTON,)),
                dma((NEWTON,)), dma((NEWTON, slots)), dma((NEWTON,)), dma((NEWTON,)),
            ],
            compiler_params=pltpu.CompilerParams(collective_id=0, has_side_effects=True),
        )(guess, start, bed, rate, balance, flags)

    return jax.shard_map(
        body, mesh=mesh,
        in_specs=(
            P("tm", "sx", "sy"), P("sx", "sy"), P("sx", "sy"), P("sx", "sy"),
            P("tm", "sx", "sy"), P("sx", "sy"),
        ),
        out_specs=P("tm", "sx", "sy"), check_vma=False,
    )
```

```python
import functools
import math

import jax
import jax.numpy as jnp
from jax import lax
from jax.experimental import pallas as pl
from jax.experimental.pallas import tpu as pltpu
from jax.sharding import PartitionSpec as P

NEWTON = 2
SWEEPS = 8
RING_Y = 4
ROWS = 8
LANES = 128
EXT = 3 * ROWS
GROUP = 4

circulant_weight = 0.25
time_step = 1.0
MESH = pl.DeviceIdType.MESH


def forward_modes(u, half, levels, odd):
    mid = half // 2
    out = []
    if not odd:
        even = [u[l] + u[half - l] for l in range(1, mid)]
        diff = [u[l] - u[half - l] for l in range(1, mid)]
        plus, minus = u[0] + u[mid], u[0] - u[mid]
        for m in range(mid):
            real = plus if m % 2 == 0 else minus
            for l in range(1, mid):
                real = real + even[l - 1] * math.cos(2 * math.pi * l * m / half)
            if m == 0:
                imag = plus if mid % 2 == 0 else minus
                for l in range(1, mid):
                    imag = imag + even[l - 1] * (-1.0) ** l
            else:
                imag = None
                for l in range(1, mid):
                    term = diff[l - 1] * -math.sin(2 * math.pi * l * m / half)
                    imag = term if imag is None else imag + term
            out.append((real, imag))
    else:
        diff = [u[l] - u[half - l] for l in range(1, mid)]
        both = [u[l] + u[half - l] for l in range(1, mid)]
        for m in range(mid):
            k = 2 * m + 1
            real = u[0]
            imag = u[mid] * -math.sin(math.pi * k / 2)
            for l in range(1, mid):
                real = real + diff[l - 1] * math.cos(2 * math.pi * l * k / levels)
                imag = imag + both[l - 1] * -math.sin(2 * math.pi * l * k / levels)
            out.append((real, imag))
    return out


def inverse_modes(v, half, levels, odd):
    mid = half // 2
    out = [None] * half
    scale = 2.0 / levels
    for l in range(mid + 1):
        if not odd:
            cosine = v[0] * (1.0 / levels) + v[1] * ((-1.0) ** l / levels)
            sine = None
            for m in range(1, mid):
                cosine = cosine + v[2 * m] * (scale * math.cos(2 * math.pi * l * m / half))
                if l not in (0, mid):
                    term = v[2 * m + 1] * (scale * math.sin(2 * math.pi * l * m / half))
                    sine = term if sine is None else sine + term
            low = cosine if sine is None else cosine - sine
            high = cosine if sine is None else cosine + sine
        else:
            cosine = sine = None
            for m in range(mid):
                k = 2 * m + 1
                term = v[2 * m] * (scale * math.cos(2 * math.pi * l * k / levels))
                cosine = term if cosine is None else cosine + term
                if l > 0:
                    term = v[2 * m + 1] * (scale * math.sin(2 * math.pi * l * k / levels))
                    sine = term if sine is None else sine + term
            low = cosine if sine is None else cosine - sine
            high = -cosine if sine is None else -cosine - sine
        out[l] = low
        if 0 < l < half:
            out[half - l] = high if l != mid else low
    return out


def kernel(
    levels, stripes,
    guess_ref, start_ref, bed_ref, rate_ref, balance_ref, flags_ref,
    out_ref,
    guess, balance, bed_in, rate_in, flags_in,
    own, edge, mass, stat_send, stat, row_send, rows,
    dsend, dext, resid, ysend, yext, coef, mean_pad, weight, work, modes, parts, dummy,
    load_sem, gsend, grecv, bsend, brecv, ssend, srecv, osend, orecv,
    esend, erecv, hsend, hrecv, dsem_s, dsem_r, ysem_s, ysem_r,
    psem_s, psem_r, qsem_s, qsem_r,
):
    half = levels // 2
    slots = half // 2
    ring_z = levels // RING_Y
    tiles = stripes * levels
    root = circulant_weight ** (1.0 / levels)
    group = min(GROUP, slots)

    level = lax.axis_index("tm")
    sx = lax.axis_index("sx")
    core = lax.axis_index("sy")
    other = 1 - core

    def turned(stripe, index):
        return index ^ ((stripe & 1) * (levels - 1))

    def snake(index):
        return index ^ (((index >> 2) & 1) * (RING_Y - 1))

    def tile_of(stripe, tm):
        return turned(stripe, snake(tm))

    def owner_of(stripe, tile):
        return snake(turned(stripe, tile))

    tile = tile_of(sx, level)
    strip = sx * levels + tile
    above = (strip + tiles - 1) & (tiles - 1)
    below = (strip + 1) & (tiles - 1)
    above_sx, below_sx = lax.div(above, levels), lax.div(below, levels)
    above_tm = owner_of(above_sx, above & (levels - 1))
    below_tm = owner_of(below_sx, below & (levels - 1))
    has_above = strip > 0
    has_below = strip < tiles - 1

    def reach(code, ring):
        return -sum(min((p ^ code) - p & ring - 1, p - (p ^ code) & ring - 1) for p in range(ring))

    far_z = sorted(range(ring_z), key=lambda code: reach(code, ring_z))
    far_y = sorted(range(RING_Y), key=lambda code: reach(code, RING_Y))
    peers = [level ^ (z * RING_Y + y) for z in far_z for y in far_y if z or y]

    def send(src, dst, ssem, rsem, device):
        pltpu.make_async_remote_copy(
            src_ref=src, dst_ref=dst, send_sem=ssem, recv_sem=rsem,
            device_id=device, device_id_type=MESH,
        ).start()

    def wait(sem, count):
        view = dummy.at[pl.ds(0, count)]
        pltpu.make_async_copy(view, view, sem).wait()

    def around(src, place, ssem, rsem):
        for to in range(2):
            send(src, place(2), ssem, rsem, (above_tm, above_sx, to))
            send(src, place(0), ssem, rsem, (below_tm, below_sx, to))
        send(src, place(1), ssem, rsem, (level, sx, other))

    barrier = pltpu.get_barrier_semaphore()

    def greet(device):
        pl.semaphore_signal(barrier, inc=1, device_id=device, device_id_type=MESH)

    for peer in peers:
        greet((peer, sx, core))
    greet((level, sx, other))
    for to in range(2):
        greet((above_tm, above_sx, to))
        greet((below_tm, below_sx, to))

    here = pl.ds(pl.multiple_of(tile * ROWS, ROWS), ROWS)
    loads = [
        pltpu.make_async_copy(guess_ref.at[0], guess, load_sem.at[0]),
        pltpu.make_async_copy(balance_ref.at[0], balance, load_sem.at[1]),
        pltpu.make_async_copy(bed_ref.at[here], bed_in, load_sem.at[2]),
        pltpu.make_async_copy(rate_ref.at[here], rate_in, load_sem.at[3]),
        pltpu.make_async_copy(flags_ref.at[here], flags_in, load_sem.at[4]),
        pltpu.make_async_copy(start_ref.at[here], own.at[0, core], load_sem.at[5]),
    ]
    for load in loads:
        load.start()
    row8 = lax.broadcasted_iota(jnp.int32, (ROWS, LANES), 0)
    lane = lax.broadcasted_iota(jnp.int32, (ROWS, LANES), 1)
    first_row, last_row = row8 == 0, row8 == ROWS - 1
    first_lane, last_lane = lane == 0, lane == LANES - 1
    row24 = lax.broadcasted_iota(jnp.int32, (EXT, LANES), 0)
    lane24 = lax.broadcasted_iota(jnp.int32, (EXT, LANES), 1)
    first24, last24 = lane24 == 0, lane24 == LANES - 1
    edge_valid = (last_row & has_above) | (first_row & has_below)
    valid24 = ((row24 >= ROWS) | has_above) & ((row24 < 2 * ROWS) | has_below)
    zero = jnp.zeros((ROWS, LANES), jnp.float32)
    for h in range(2):
        for pad in (pl.ds(0, ROWS), pl.ds(ROWS + EXT, ROWS)):
            mean_pad[h, pad] = zero
            for turn in range(2):
                for slot in range(group):
                    for i in range(2):
                        work[turn, slot, i, h, pad] = zero
    for load in loads:
        load.wait()

    inside_own = (flags_in[...] != 0).astype(jnp.float32)
    boost = 1.0 + (flags_in[...] == 2).astype(jnp.float32)
    cst_own = inside_own * boost * rate_in[...]
    bed_own = bed_in[...]
    for i, value in enumerate((cst_own, bed_own, inside_own)):
        stat_send[i] = value
        stat[i, core, ROWS : 2 * ROWS] = value

    pl.semaphore_wait(barrier, levels - 1 + 5)

    def scatter(src, dst, ssem, rsem):
        for peer in peers:
            rows_to = pl.ds(pl.multiple_of(tile_of(sx, peer) * ROWS, ROWS), ROWS)
            send(src.at[rows_to], dst, ssem, rsem, (peer, sx, core))

    scatter(guess, own.at[1 + level, core], gsend, grecv)
    scatter(balance, mass.at[level], bsend, brecv)
    around(stat_send, lambda p: stat.at[:, core, pl.ds(p * ROWS, ROWS)], ssend, srecv)
    own[1 + level, core] = guess[here]
    mass[level] = balance[here]

    wait(grecv, levels - 1)
    mine = own.at[pl.ds(1, levels), core]
    send(mine, mine, hsend, hrecv, (level, sx, other))
    for l in range(levels):
        row_send[0, l : l + 1] = own[1 + l, core, 0:1]
        row_send[1, l : l + 1] = own[1 + l, core, ROWS - 1 : ROWS]
    send(row_send.at[0], rows.at[1], esend, erecv, (above_tm, above_sx, core))
    send(row_send.at[1], rows.at[0], esend, erecv, (below_tm, below_sx, core))

    def neighbours(x, x_other, x_edge):
        right = pltpu.roll(jnp.where(first_lane, jnp.where(core == 0, x_other, 0.0), x), LANES - 1, 1)
        left = pltpu.roll(jnp.where(last_lane, jnp.where(core == 1, x_other, 0.0), x), 1, 1)
        down = pltpu.roll(jnp.where(first_row, x_edge, x), ROWS - 1, 0)
        up = pltpu.roll(jnp.where(last_row, x_edge, x), 1, 0)
        return right, left, down, up

    wait(srecv, 3 * 5)
    wait(erecv, 2 * (levels // ROWS))
    for l in range(levels):
        edge[l] = jnp.where(last_row, rows[0, l : l + 1], rows[1, l : l + 1])

    cst_other = stat[0, other, ROWS : 2 * ROWS]
    bed_other = stat[1, other, ROWS : 2 * ROWS]
    cst_edge = jnp.where(
        edge_valid, jnp.where(last_row, stat[0, core, 0:ROWS], stat[0, core, 2 * ROWS :]), 0.0
    )
    bed_edge = jnp.where(last_row, stat[1, core, 0:ROWS], stat[1, core, 2 * ROWS :])

    wait(hrecv, levels)

    def diffusivity(scale, h):
        return scale * h * h * jnp.abs(h)

    def newton(n, carry):
        more = n < NEWTON - 1

        sums = [zero, zero, zero]
        for l in range(levels):
            sums[0] = sums[0] + diffusivity(cst_own, own[1 + l, core])
            sums[1] = sums[1] + diffusivity(cst_other, own[1 + l, other])
            sums[2] = sums[2] + diffusivity(cst_edge, edge[l])
        mean, mean_other, mean_edge = (s * (1.0 / levels) for s in sums)
        total = 0.5 * (4.0 * mean + sum(neighbours(mean, mean_other, mean_edge)))
        for i, value in enumerate((mean, total)):
            dsend[n, i] = value
            dext[n, i, core, ROWS : 2 * ROWS] = value
        around(
            dsend.at[n], lambda p: dext.at[n, :, core, pl.ds(p * ROWS, ROWS)],
            dsem_s.at[n], dsem_r.at[n],
        )

        @pl.when(n == 0)
        def _():
            wait(brecv, levels - 1)

        for l in range(levels):
            h, h_other, h_edge = own[1 + l, core], own[1 + l, other], edge[l]
            s = h + bed_own
            d_near = neighbours(
                diffusivity(cst_own, h), diffusivity(cst_other, h_other),
                diffusivity(cst_edge, h_edge),
            )
            s_near = neighbours(
                s, h_other + bed_other, jnp.where(edge_valid, h_edge + bed_edge, 0.0)
            )
            d = diffusivity(cst_own, h)
            flux = sum((d + dn) * (s - sn) for dn, sn in zip(d_near, s_near))
            change = (h - own[l, core]) / time_step + 0.5 * flux - mass[l]
            resid[l] = inside_own * change * (root ** l)

        low = [resid[l] for l in range(half)]
        high = [resid[l + half] for l in range(half)]
        evens = forward_modes([a + b for a, b in zip(low, high)], half, levels, False)
        odds = forward_modes([a - b for a, b in zip(low, high)], half, levels, True)
        for slot in range(slots):
            for i in range(2):
                ysend[n, 0, 2 * slot + i] = evens[slot][i]
                ysend[n, 1, 2 * slot + i] = odds[slot][i]
                yext[n, 2 * slot + i, core, ROWS : 2 * ROWS] = jnp.where(
                    core == 0, evens[slot][i], odds[slot][i]
                )
            pair = pl.ds(2 * slot, 2)

            def place(p):
                return yext.at[n, pair, core, pl.ds(p * ROWS, ROWS)]

            s_sem, r_sem = ysem_s.at[n], ysem_r.at[n, slot]
            for to in range(2):
                send(ysend.at[n, to, pair], place(2), s_sem, r_sem, (above_tm, above_sx, to))
                send(ysend.at[n, to, pair], place(0), s_sem, r_sem, (below_tm, below_sx, to))
            send(ysend.at[n, other, pair], place(1), s_sem, r_sem, (level, sx, other))

        wait(dsem_r.at[n], 2 * 5)
        inner = pl.ds(ROWS, EXT)
        m0, m1 = (jnp.where(valid24, dext[n, 0, h], 0.0) for h in range(2))
        mean_pad[0, inner] = m0
        mean_pad[1, inner] = m1
        weight[0, 0] = 0.5 * (m0 + pltpu.roll(jnp.where(first24, m1, m0), LANES - 1, 1))
        weight[0, 1] = jnp.where(last24, 0.0, 0.5 * (m1 + pltpu.roll(m1, LANES - 1, 1)))
        weight[1, 0] = jnp.where(first24, 0.0, 0.5 * (m0 + pltpu.roll(m0, 1, 1)))
        weight[1, 1] = 0.5 * (m1 + pltpu.roll(jnp.where(last24, m0, m1), 1, 1))
        for h, m in ((0, m0), (1, m1)):
            weight[2, h] = 0.5 * (m + mean_pad[h, pl.ds(ROWS + 1, EXT)])
            weight[3, h] = 0.5 * (m + mean_pad[h, pl.ds(ROWS - 1, EXT)])

        def shift(k):
            angle = 2 * math.pi * k / levels
            return (
                (1.0 - root * math.cos(angle)) / time_step,
                root * math.sin(angle) / time_step,
            )

        for m in range(slots):
            even_real, even_imag = shift(2 * m)
            odd_real, odd_imag = shift(2 * m + 1)
            last_real = shift(half)[0] if m == 0 else even_real
            imag = jnp.where(core == 0, 0.0 if m == 0 else even_imag, odd_imag)
            for h in range(2):
                inside = jnp.where(valid24, stat[2, h], 0.0)
                real = dext[n, 1, h] + jnp.where(core == 0, even_real, odd_real)
                scaled = inside / (real * real + imag * imag)
                coef[m, 0, h] = scaled * real
                coef[m, 1, h] = scaled * -imag
                if m == 0:
                    real = dext[n, 1, h] + jnp.where(core == 0, last_real, odd_real)
                    coef[m, 2, h] = inside * real / (real * real + imag * imag)
                else:
                    coef[m, 2, h] = scaled * real

        def solve(g, carry):
            for i in range(group):
                wait(ysem_r.at[n, g * group + i], 2 * 5)

            def apply(slot, h, real, imag):
                a, b, c = (coef[slot, k, h] for k in range(3))
                return real * a - imag * b, real * b + imag * c

            for i in range(group):
                slot = g * group + i
                for h in range(2):
                    value = apply(slot, h, yext[n, 2 * slot, h], yext[n, 2 * slot + 1, h])
                    for part in range(2):
                        work[0, i, part, h, inner] = value[part]
            for sweep in range(SWEEPS - 1):
                now, then = sweep % 2, (sweep + 1) % 2
                for i in range(group):
                    slot = g * group + i
                    spread = []
                    for part in range(2):
                        v0, v1 = work[now, i, part, 0, inner], work[now, i, part, 1, inner]
                        right = (
                            pltpu.roll(jnp.where(first24, v1, v0), LANES - 1, 1),
                            pltpu.roll(v1, LANES - 1, 1),
                        )
                        left = (
                            pltpu.roll(v0, 1, 1),
                            pltpu.roll(jnp.where(last24, v0, v1), 1, 1),
                        )
                        spread.append([
                            weight[0, h] * right[h] + weight[1, h] * left[h]
                            + weight[2, h] * work[now, i, part, h, pl.ds(ROWS + 1, EXT)]
                            + weight[3, h] * work[now, i, part, h, pl.ds(ROWS - 1, EXT)]
                            for h in range(2)
                        ])
                    for h in range(2):
                        value = apply(
                            slot, h, yext[n, 2 * slot, h] + spread[0][h],
                            yext[n, 2 * slot + 1, h] + spread[1][h],
                        )
                        for part in range(2):
                            v = value[part]
                            if sweep < SWEEPS - 2:
                                work[then, i, part, h, inner] = v
                            else:
                                modes[h, 2 * slot + part] = v[ROWS : 2 * ROWS]
                                modes[2 + h, 2 * slot + part] = jnp.where(
                                    last_row, v[0:ROWS], v[2 * ROWS :]
                                )
            return carry

        lax.fori_loop(0, slots // group, solve, 0)

        for parity in range(2):
            @pl.when(core == parity)
            def _():
                def invert(i, carry):
                    p = (i & 2) + jnp.where((i & 1) == 0, other, core)
                    values = inverse_modes(
                        [modes[p, f] for f in range(half)], half, levels, parity == 1
                    )
                    for l in range(half):
                        parts[n, parity, p, l] = values[l]
                    block = parts.at[n, parity, p]

                    @pl.when(i == 0)
                    def _():
                        send(block, block, psem_s.at[n], psem_r.at[n], (level, sx, other))

                    @pl.when((i > 0) & (i < 3) & more)
                    def _():
                        send(block, block, qsem_s, qsem_r, (level, sx, other))

                    return carry

                lax.fori_loop(0, jnp.where(more, 4, 2), invert, 0)

        @pl.when(n == 0)
        def _():
            wait(hsend, levels)

        def update(target, p):
            for l in range(half):
                drop = root ** -l
                even, odd = parts[n, 0, p, l], parts[n, 1, p, l]
                near, far = target(l), target(l + half)
                near[...] = near[...] - (even + odd) * drop
                far[...] = far[...] - (even - odd) * (drop * root ** -half)

        wait(psem_r.at[n], half)
        update(lambda l: own.at[1 + l, core], core)

        @pl.when(more)
        def _():
            wait(qsem_r, 2 * half)
            update(lambda l: own.at[1 + l, other], other)
            update(lambda l: edge.at[l], 2 + core)

        return carry

    lax.fori_loop(0, NEWTON, newton, 0)

    for peer in peers:
        send(own.at[1 + peer, core], out_ref.at[0, here], osend, orecv, (peer, sx, core))
    out_ref[0, here] = own[1 + level, core]

    wait(gsend, levels - 1)
    wait(bsend, levels - 1)
    wait(ssend, 3 * 5)
    wait(esend, 2 * (levels // ROWS))
    for n in range(NEWTON):
        wait(dsem_s.at[n], 2 * 5)
        wait(ysem_s.at[n], 2 * 5 * slots)
        wait(psem_s.at[n], half)
    if NEWTON > 1:
        wait(qsem_s, 2 * half * (NEWTON - 1))
    wait(osend, levels - 1)
    wait(orecv, levels - 1)


def solution(mesh):
    levels, stripes = mesh.shape["tm"], mesh.shape["sx"]
    half = levels // 2
    slots = half // 2
    tile = (ROWS, LANES)
    wide = (EXT, LANES)
    padded = (EXT + 2 * ROWS, LANES)
    f32 = jnp.float32

    def vmem(*lead, last=tile, dtype=f32):
        return pltpu.VMEM((*lead, *last), dtype)

    dma = pltpu.SemaphoreType.DMA

    def body(guess, start, bed, rate, balance, flags):
        rows = guess.shape[1]
        return pl.pallas_call(
            functools.partial(kernel, levels, stripes),
            out_shape=jax.ShapeDtypeStruct(guess.shape, f32),
            in_specs=[pl.BlockSpec(memory_space=pl.ANY)] * 6,
            out_specs=pl.BlockSpec(memory_space=pltpu.VMEM),
            scratch_shapes=[
                vmem(last=(rows, LANES)), vmem(last=(rows, LANES)),
                vmem(), vmem(), vmem(dtype=jnp.int32),
                vmem(levels + 1, 2), vmem(levels), vmem(levels),
                vmem(3), vmem(3, 2, last=wide),
                vmem(2, last=(levels, LANES)), vmem(2, last=(levels, LANES)),
                vmem(NEWTON, 2), vmem(NEWTON, 2, 2, last=wide),
                vmem(levels), vmem(NEWTON, 2, half),
                vmem(NEWTON, half, 2, last=wide),
                vmem(slots, 3, 2, last=wide), vmem(2, last=padded), vmem(4, 2, last=wide),
                vmem(2, min(GROUP, slots), 2, 2, last=padded),
                vmem(4, half), vmem(NEWTON, 2, 4, half),
                vmem(max(2 * 5 * slots, 4 * half, levels)),
                dma((6,)), dma, dma, dma, dma, dma, dma, dma, dma,
                dma, dma, dma, dma, dma((NEWTON,)), dma((NEWTON,)),
                dma((NEWTON,)), dma((NEWTON, slots)), dma((NEWTON,)), dma((NEWTON,)), dma, dma,
            ],
            compiler_params=pltpu.CompilerParams(collective_id=0, has_side_effects=True),
        )(guess, start, bed, rate, balance, flags)

    return jax.shard_map(
        body, mesh=mesh,
        in_specs=(
            P("tm", "sx", "sy"), P("sx", "sy"), P("sx", "sy"), P("sx", "sy"),
            P("tm", "sx", "sy"), P("sx", "sy"),
        ),
        out_specs=P("tm", "sx", "sy"), check_vma=False,
    )
```

```python
import functools
import math

import jax
import jax.numpy as jnp
from jax import lax
from jax.experimental import pallas as pl
from jax.experimental.pallas import tpu as pltpu
from jax.sharding import PartitionSpec as P

NEWTON = 2
SWEEPS = 8
RING_Y = 4
ROWS = 8
LANES = 128
EXT = 3 * ROWS
GROUP = 4

circulant_weight = 0.25
time_step = 1.0
MESH = pl.DeviceIdType.MESH


def forward_modes(u, half, levels, odd):
    mid = half // 2
    out = []
    if not odd:
        even = [u[l] + u[half - l] for l in range(1, mid)]
        diff = [u[l] - u[half - l] for l in range(1, mid)]
        plus, minus = u[0] + u[mid], u[0] - u[mid]
        for m in range(mid):
            real = plus if m % 2 == 0 else minus
            for l in range(1, mid):
                real = real + even[l - 1] * math.cos(2 * math.pi * l * m / half)
            if m == 0:
                imag = plus if mid % 2 == 0 else minus
                for l in range(1, mid):
                    imag = imag + even[l - 1] * (-1.0) ** l
            else:
                imag = None
                for l in range(1, mid):
                    term = diff[l - 1] * -math.sin(2 * math.pi * l * m / half)
                    imag = term if imag is None else imag + term
            out.append((real, imag))
    else:
        diff = [u[l] - u[half - l] for l in range(1, mid)]
        both = [u[l] + u[half - l] for l in range(1, mid)]
        for m in range(mid):
            k = 2 * m + 1
            real = u[0]
            imag = u[mid] * -math.sin(math.pi * k / 2)
            for l in range(1, mid):
                real = real + diff[l - 1] * math.cos(2 * math.pi * l * k / levels)
                imag = imag + both[l - 1] * -math.sin(2 * math.pi * l * k / levels)
            out.append((real, imag))
    return out


def inverse_modes(v, half, levels, odd):
    mid = half // 2
    out = [None] * half
    scale = 2.0 / levels
    for l in range(mid + 1):
        if not odd:
            cosine = v[0] * (1.0 / levels) + v[1] * ((-1.0) ** l / levels)
            sine = None
            for m in range(1, mid):
                cosine = cosine + v[2 * m] * (scale * math.cos(2 * math.pi * l * m / half))
                if l not in (0, mid):
                    term = v[2 * m + 1] * (scale * math.sin(2 * math.pi * l * m / half))
                    sine = term if sine is None else sine + term
            low = cosine if sine is None else cosine - sine
            high = cosine if sine is None else cosine + sine
        else:
            cosine = sine = None
            for m in range(mid):
                k = 2 * m + 1
                term = v[2 * m] * (scale * math.cos(2 * math.pi * l * k / levels))
                cosine = term if cosine is None else cosine + term
                if l > 0:
                    term = v[2 * m + 1] * (scale * math.sin(2 * math.pi * l * k / levels))
                    sine = term if sine is None else sine + term
            low = cosine if sine is None else cosine - sine
            high = -cosine if sine is None else -cosine - sine
        out[l] = low
        if 0 < l < half:
            out[half - l] = high if l != mid else low
    return out


def kernel(
    levels, stripes,
    guess_ref, start_ref, bed_ref, rate_ref, balance_ref, flags_ref,
    out_ref,
    guess, balance, bed_in, rate_in, flags_in,
    own, edge, mass, stat_send, stat, row_send, rows,
    dsend, dext, resid, ysend, yext, coef, mean_pad, weight, work, modes, parts, dummy,
    load_sem, gsend, grecv, bsend, brecv, ssend, srecv, osend, orecv,
    esend, erecv, hsend, hrecv, dsem_s, dsem_r, ysem_s, ysem_r,
    psem_s, psem_r, qsem_s, qsem_r,
):
    half = levels // 2
    slots = half // 2
    ring_z = levels // RING_Y
    tiles = stripes * levels
    root = circulant_weight ** (1.0 / levels)
    group = min(GROUP, slots)

    level = lax.axis_index("tm")
    sx = lax.axis_index("sx")
    core = lax.axis_index("sy")
    other = 1 - core

    def turned(stripe, index):
        return index ^ ((stripe & 1) * (levels - 1))

    def snake(index):
        return index ^ (((index >> 2) & 1) * (RING_Y - 1))

    def tile_of(stripe, tm):
        return turned(stripe, snake(tm))

    def owner_of(stripe, tile):
        return snake(turned(stripe, tile))

    tile = tile_of(sx, level)
    strip = sx * levels + tile
    above = (strip + tiles - 1) & (tiles - 1)
    below = (strip + 1) & (tiles - 1)
    above_sx, below_sx = lax.div(above, levels), lax.div(below, levels)
    above_tm = owner_of(above_sx, above & (levels - 1))
    below_tm = owner_of(below_sx, below & (levels - 1))
    has_above = strip > 0
    has_below = strip < tiles - 1

    def reach(code, ring):
        return -sum(min((p ^ code) - p & ring - 1, p - (p ^ code) & ring - 1) for p in range(ring))

    far_z = sorted(range(ring_z), key=lambda code: reach(code, ring_z))
    far_y = sorted(range(RING_Y), key=lambda code: reach(code, RING_Y))
    peers = [level ^ (z * RING_Y + y) for z in far_z for y in far_y if z or y]

    def send(src, dst, ssem, rsem, device):
        pltpu.make_async_remote_copy(
            src_ref=src, dst_ref=dst, send_sem=ssem, recv_sem=rsem,
            device_id=device, device_id_type=MESH,
        ).start()

    def wait(sem, count):
        view = dummy.at[pl.ds(0, count)]
        pltpu.make_async_copy(view, view, sem).wait()

    def around(src, place, ssem, rsem):
        for to in range(2):
            send(src, place(2), ssem, rsem, (above_tm, above_sx, to))
            send(src, place(0), ssem, rsem, (below_tm, below_sx, to))
        send(src, place(1), ssem, rsem, (level, sx, other))

    barrier = pltpu.get_barrier_semaphore()

    def greet(device):
        pl.semaphore_signal(barrier, inc=1, device_id=device, device_id_type=MESH)

    for peer in peers:
        greet((peer, sx, core))
    greet((level, sx, other))
    for to in range(2):
        greet((above_tm, above_sx, to))
        greet((below_tm, below_sx, to))

    here = pl.ds(pl.multiple_of(tile * ROWS, ROWS), ROWS)
    loads = [
        pltpu.make_async_copy(guess_ref.at[0], guess, load_sem.at[0]),
        pltpu.make_async_copy(balance_ref.at[0], balance, load_sem.at[1]),
        pltpu.make_async_copy(bed_ref.at[here], bed_in, load_sem.at[2]),
        pltpu.make_async_copy(rate_ref.at[here], rate_in, load_sem.at[3]),
        pltpu.make_async_copy(flags_ref.at[here], flags_in, load_sem.at[4]),
        pltpu.make_async_copy(start_ref.at[here], own.at[0, core], load_sem.at[5]),
    ]
    for load in loads:
        load.start()
    row8 = lax.broadcasted_iota(jnp.int32, (ROWS, LANES), 0)
    lane = lax.broadcasted_iota(jnp.int32, (ROWS, LANES), 1)
    first_row, last_row = row8 == 0, row8 == ROWS - 1
    first_lane, last_lane = lane == 0, lane == LANES - 1
    row24 = lax.broadcasted_iota(jnp.int32, (EXT, LANES), 0)
    lane24 = lax.broadcasted_iota(jnp.int32, (EXT, LANES), 1)
    first24, last24 = lane24 == 0, lane24 == LANES - 1
    edge_valid = (last_row & has_above) | (first_row & has_below)
    valid24 = ((row24 >= ROWS) | has_above) & ((row24 < 2 * ROWS) | has_below)
    zero = jnp.zeros((ROWS, LANES), jnp.float32)
    for h in range(2):
        for pad in (pl.ds(0, ROWS), pl.ds(ROWS + EXT, ROWS)):
            mean_pad[h, pad] = zero
            for turn in range(2):
                for slot in range(group):
                    for i in range(2):
                        work[turn, slot, i, h, pad] = zero
    for load in loads:
        load.wait()

    inside_own = (flags_in[...] != 0).astype(jnp.float32)
    boost = 1.0 + (flags_in[...] == 2).astype(jnp.float32)
    cst_own = inside_own * boost * rate_in[...]
    bed_own = bed_in[...]
    for i, value in enumerate((cst_own, bed_own, inside_own)):
        stat_send[i] = value
        stat[i, core, ROWS : 2 * ROWS] = value

    pl.semaphore_wait(barrier, levels - 1 + 5)

    def scatter(src, dst, ssem, rsem):
        for peer in peers:
            rows_to = pl.ds(pl.multiple_of(tile_of(sx, peer) * ROWS, ROWS), ROWS)
            send(src.at[rows_to], dst, ssem, rsem, (peer, sx, core))

    scatter(guess, own.at[1 + level, core], gsend, grecv)
    scatter(balance, mass.at[level], bsend, brecv)
    around(stat_send, lambda p: stat.at[:, core, pl.ds(p * ROWS, ROWS)], ssend, srecv)
    own[1 + level, core] = guess[here]
    mass[level] = balance[here]

    wait(grecv, levels - 1)
    mine = own.at[pl.ds(1, levels), core]
    send(mine, mine, hsend, hrecv, (level, sx, other))
    for l in range(levels):
        row_send[0, l : l + 1] = own[1 + l, core, 0:1]
        row_send[1, l : l + 1] = own[1 + l, core, ROWS - 1 : ROWS]
    send(row_send.at[0], rows.at[1], esend, erecv, (above_tm, above_sx, core))
    send(row_send.at[1], rows.at[0], esend, erecv, (below_tm, below_sx, core))

    def neighbours(x, x_other, x_edge):
        right = pltpu.roll(jnp.where(first_lane, jnp.where(core == 0, x_other, 0.0), x), LANES - 1, 1)
        left = pltpu.roll(jnp.where(last_lane, jnp.where(core == 1, x_other, 0.0), x), 1, 1)
        down = pltpu.roll(jnp.where(first_row, x_edge, x), ROWS - 1, 0)
        up = pltpu.roll(jnp.where(last_row, x_edge, x), 1, 0)
        return right, left, down, up

    wait(srecv, 3 * 5)
    wait(erecv, 2 * (levels // ROWS))
    for l in range(levels):
        edge[l] = jnp.where(last_row, rows[0, l : l + 1], rows[1, l : l + 1])

    cst_other = stat[0, other, ROWS : 2 * ROWS]
    bed_other = stat[1, other, ROWS : 2 * ROWS]
    cst_edge = jnp.where(
        edge_valid, jnp.where(last_row, stat[0, core, 0:ROWS], stat[0, core, 2 * ROWS :]), 0.0
    )
    bed_edge = jnp.where(last_row, stat[1, core, 0:ROWS], stat[1, core, 2 * ROWS :])

    wait(hrecv, levels)

    def diffusivity(scale, h):
        return scale * h * h * jnp.abs(h)

    def newton(n, carry):
        more = n < NEWTON - 1

        sums = [zero, zero, zero]
        for l in range(levels):
            sums[0] = sums[0] + diffusivity(cst_own, own[1 + l, core])
            sums[1] = sums[1] + diffusivity(cst_other, own[1 + l, other])
            sums[2] = sums[2] + diffusivity(cst_edge, edge[l])
        mean, mean_other, mean_edge = (s * (1.0 / levels) for s in sums)
        total = 0.5 * (4.0 * mean + sum(neighbours(mean, mean_other, mean_edge)))
        for i, value in enumerate((mean, total)):
            dsend[n, i] = value
            dext[n, i, core, ROWS : 2 * ROWS] = value
        around(
            dsend.at[n], lambda p: dext.at[n, :, core, pl.ds(p * ROWS, ROWS)],
            dsem_s.at[n], dsem_r.at[n],
        )

        @pl.when(n == 0)
        def _():
            wait(brecv, levels - 1)

        for l in range(levels):
            h, h_other, h_edge = own[1 + l, core], own[1 + l, other], edge[l]
            s = h + bed_own
            d_near = neighbours(
                diffusivity(cst_own, h), diffusivity(cst_other, h_other),
                diffusivity(cst_edge, h_edge),
            )
            s_near = neighbours(
                s, h_other + bed_other, jnp.where(edge_valid, h_edge + bed_edge, 0.0)
            )
            d = diffusivity(cst_own, h)
            flux = sum((d + dn) * (s - sn) for dn, sn in zip(d_near, s_near))
            change = (h - own[l, core]) / time_step + 0.5 * flux - mass[l]
            resid[l] = inside_own * change * (root ** l)

        low = [resid[l] for l in range(half)]
        high = [resid[l + half] for l in range(half)]
        evens = forward_modes([a + b for a, b in zip(low, high)], half, levels, False)
        odds = forward_modes([a - b for a, b in zip(low, high)], half, levels, True)
        for slot in range(slots):
            for i in range(2):
                ysend[n, 0, 2 * slot + i] = evens[slot][i]
                ysend[n, 1, 2 * slot + i] = odds[slot][i]
                yext[n, 2 * slot + i, core, ROWS : 2 * ROWS] = jnp.where(
                    core == 0, evens[slot][i], odds[slot][i]
                )
            pair = pl.ds(2 * slot, 2)

            def place(p):
                return yext.at[n, pair, core, pl.ds(p * ROWS, ROWS)]

            s_sem, r_sem = ysem_s.at[n], ysem_r.at[n, slot]
            for to in range(2):
                send(ysend.at[n, to, pair], place(2), s_sem, r_sem, (above_tm, above_sx, to))
                send(ysend.at[n, to, pair], place(0), s_sem, r_sem, (below_tm, below_sx, to))
            send(ysend.at[n, other, pair], place(1), s_sem, r_sem, (level, sx, other))

        wait(dsem_r.at[n], 2 * 5)
        inner = pl.ds(ROWS, EXT)
        m0, m1 = (jnp.where(valid24, dext[n, 0, h], 0.0) for h in range(2))
        mean_pad[0, inner] = m0
        mean_pad[1, inner] = m1
        weight[0, 0] = 0.5 * (m0 + pltpu.roll(jnp.where(first24, m1, m0), LANES - 1, 1))
        weight[0, 1] = jnp.where(last24, 0.0, 0.5 * (m1 + pltpu.roll(m1, LANES - 1, 1)))
        weight[1, 0] = jnp.where(first24, 0.0, 0.5 * (m0 + pltpu.roll(m0, 1, 1)))
        weight[1, 1] = 0.5 * (m1 + pltpu.roll(jnp.where(last24, m0, m1), 1, 1))
        for h, m in ((0, m0), (1, m1)):
            weight[2, h] = 0.5 * (m + mean_pad[h, pl.ds(ROWS + 1, EXT)])
            weight[3, h] = 0.5 * (m + mean_pad[h, pl.ds(ROWS - 1, EXT)])

        def shift(k):
            angle = 2 * math.pi * k / levels
            return (
                (1.0 - root * math.cos(angle)) / time_step,
                root * math.sin(angle) / time_step,
            )

        for m in range(slots):
            even_real, even_imag = shift(2 * m)
            odd_real, odd_imag = shift(2 * m + 1)
            last_real = shift(half)[0] if m == 0 else even_real
            imag = jnp.where(core == 0, 0.0 if m == 0 else even_imag, odd_imag)
            for h in range(2):
                inside = jnp.where(valid24, stat[2, h], 0.0)
                real = dext[n, 1, h] + jnp.where(core == 0, even_real, odd_real)
                scaled = inside / (real * real + imag * imag)
                coef[m, 0, h] = scaled * real
                coef[m, 1, h] = scaled * -imag
                if m == 0:
                    real = dext[n, 1, h] + jnp.where(core == 0, last_real, odd_real)
                    coef[m, 2, h] = inside * real / (real * real + imag * imag)
                else:
                    coef[m, 2, h] = scaled * real

        def solve(g, carry):
            for i in range(group):
                wait(ysem_r.at[n, g * group + i], 2 * 5)

            def apply(slot, h, real, imag):
                a, b, c = (coef[slot, k, h] for k in range(3))
                return real * a - imag * b, real * b + imag * c

            for i in range(group):
                slot = g * group + i
                for h in range(2):
                    value = apply(slot, h, yext[n, 2 * slot, h], yext[n, 2 * slot + 1, h])
                    for part in range(2):
                        work[0, i, part, h, inner] = value[part]
            for sweep in range(SWEEPS - 1):
                now, then = sweep % 2, (sweep + 1) % 2
                for i in range(group):
                    slot = g * group + i
                    spread = []
                    for part in range(2):
                        v0, v1 = work[now, i, part, 0, inner], work[now, i, part, 1, inner]
                        right = (
                            pltpu.roll(jnp.where(first24, v1, v0), LANES - 1, 1),
                            pltpu.roll(v1, LANES - 1, 1),
                        )
                        left = (
                            pltpu.roll(v0, 1, 1),
                            pltpu.roll(jnp.where(last24, v0, v1), 1, 1),
                        )
                        spread.append([
                            weight[0, h] * right[h] + weight[1, h] * left[h]
                            + weight[2, h] * work[now, i, part, h, pl.ds(ROWS + 1, EXT)]
                            + weight[3, h] * work[now, i, part, h, pl.ds(ROWS - 1, EXT)]
                            for h in range(2)
                        ])
                    for h in range(2):
                        value = apply(
                            slot, h, yext[n, 2 * slot, h] + spread[0][h],
                            yext[n, 2 * slot + 1, h] + spread[1][h],
                        )
                        for part in range(2):
                            v = value[part]
                            if sweep < SWEEPS - 2:
                                work[then, i, part, h, inner] = v
                            else:
                                modes[h, 2 * slot + part] = v[ROWS : 2 * ROWS]
                                modes[2 + h, 2 * slot + part] = jnp.where(
                                    last_row, v[0:ROWS], v[2 * ROWS :]
                                )
            return carry

        lax.fori_loop(0, slots // group, solve, 0)

        for parity in range(2):
            @pl.when(core == parity)
            def _():
                def invert(i, carry):
                    p = (i & 2) + jnp.where((i & 1) == 0, other, core)
                    values = inverse_modes(
                        [modes[p, f] for f in range(half)], half, levels, parity == 1
                    )
                    for l in range(half):
                        parts[n, parity, p, l] = values[l]
                    block = parts.at[n, parity, p]

                    @pl.when(i == 0)
                    def _():
                        send(block, block, psem_s.at[n], psem_r.at[n], (level, sx, other))

                    @pl.when((i > 0) & (i < 3) & more)
                    def _():
                        send(block, block, qsem_s, qsem_r, (level, sx, other))

                    return carry

                lax.fori_loop(0, jnp.where(more, 4, 2), invert, 0)

        @pl.when(n == 0)
        def _():
            wait(hsend, levels)

        def update(target, p):
            for l in range(half):
                drop = root ** -l
                even, odd = parts[n, 0, p, l], parts[n, 1, p, l]
                near, far = target(l), target(l + half)
                near[...] = near[...] - (even + odd) * drop
                far[...] = far[...] - (even - odd) * (drop * root ** -half)

        wait(psem_r.at[n], half)
        update(lambda l: own.at[1 + l, core], core)

        @pl.when(more)
        def _():
            wait(qsem_r, 2 * half)
            update(lambda l: own.at[1 + l, other], other)
            update(lambda l: edge.at[l], 2 + core)

        return carry

    lax.fori_loop(0, NEWTON, newton, 0)

    for peer in peers:
        send(own.at[1 + peer, core], out_ref.at[0, here], osend, orecv, (peer, sx, core))
    out_ref[0, here] = own[1 + level, core]

    wait(gsend, levels - 1)
    wait(bsend, levels - 1)
    wait(ssend, 3 * 5)
    wait(esend, 2 * (levels // ROWS))
    for n in range(NEWTON):
        wait(dsem_s.at[n], 2 * 5)
        wait(ysem_s.at[n], 2 * 5 * slots)
        wait(psem_s.at[n], half)
    if NEWTON > 1:
        wait(qsem_s, 2 * half * (NEWTON - 1))
    wait(osend, levels - 1)
    wait(orecv, levels - 1)


def solution(mesh):
    levels, stripes = mesh.shape["tm"], mesh.shape["sx"]
    half = levels // 2
    slots = half // 2
    tile = (ROWS, LANES)
    wide = (EXT, LANES)
    padded = (EXT + 2 * ROWS, LANES)
    f32 = jnp.float32

    def vmem(*lead, last=tile, dtype=f32):
        return pltpu.VMEM((*lead, *last), dtype)

    dma = pltpu.SemaphoreType.DMA

    def body(guess, start, bed, rate, balance, flags):
        rows = guess.shape[1]
        return pl.pallas_call(
            functools.partial(kernel, levels, stripes),
            out_shape=pltpu.VMEM(guess.shape, f32),
            in_specs=[pl.BlockSpec(memory_space=pl.ANY)] * 6,
            out_specs=pl.BlockSpec(memory_space=pltpu.VMEM),
            scratch_shapes=[
                vmem(last=(rows, LANES)), vmem(last=(rows, LANES)),
                vmem(), vmem(), vmem(dtype=jnp.int32),
                vmem(levels + 1, 2), vmem(levels), vmem(levels),
                vmem(3), vmem(3, 2, last=wide),
                vmem(2, last=(levels, LANES)), vmem(2, last=(levels, LANES)),
                vmem(NEWTON, 2), vmem(NEWTON, 2, 2, last=wide),
                vmem(levels), vmem(NEWTON, 2, half),
                vmem(NEWTON, half, 2, last=wide),
                vmem(slots, 3, 2, last=wide), vmem(2, last=padded), vmem(4, 2, last=wide),
                vmem(2, min(GROUP, slots), 2, 2, last=padded),
                vmem(4, half), vmem(NEWTON, 2, 4, half),
                vmem(max(2 * 5 * slots, 4 * half, levels)),
                dma((6,)), dma, dma, dma, dma, dma, dma, dma, dma,
                dma, dma, dma, dma, dma((NEWTON,)), dma((NEWTON,)),
                dma((NEWTON,)), dma((NEWTON, slots)), dma((NEWTON,)), dma((NEWTON,)), dma, dma,
            ],
            compiler_params=pltpu.CompilerParams(collective_id=0, has_side_effects=True),
        )(guess, start, bed, rate, balance, flags)

    return jax.shard_map(
        body, mesh=mesh,
        in_specs=(
            P("tm", "sx", "sy"), P("sx", "sy"), P("sx", "sy"), P("sx", "sy"),
            P("tm", "sx", "sy"), P("sx", "sy"),
        ),
        out_specs=P("tm", "sx", "sy"), check_vma=False,
    )
```

```python
import functools
import math

import jax
import jax.numpy as jnp
from jax import lax
from jax.experimental import pallas as pl
from jax.experimental.pallas import tpu as pltpu
from jax.sharding import PartitionSpec as P

NEWTON = 2
SWEEPS = 8
RING_Y = 4
ROWS = 8
LANES = 128
EXT = 3 * ROWS
GROUP = 4
CHUNK = 4

circulant_weight = 0.25
time_step = 1.0
MESH = pl.DeviceIdType.MESH


def forward_modes(u, half, levels, odd):
    mid = half // 2
    out = []
    if not odd:
        even = [u[l] + u[half - l] for l in range(1, mid)]
        diff = [u[l] - u[half - l] for l in range(1, mid)]
        plus, minus = u[0] + u[mid], u[0] - u[mid]
        for m in range(mid):
            real = plus if m % 2 == 0 else minus
            for l in range(1, mid):
                real = real + even[l - 1] * math.cos(2 * math.pi * l * m / half)
            if m == 0:
                imag = plus if mid % 2 == 0 else minus
                for l in range(1, mid):
                    imag = imag + even[l - 1] * (-1.0) ** l
            else:
                imag = None
                for l in range(1, mid):
                    term = diff[l - 1] * -math.sin(2 * math.pi * l * m / half)
                    imag = term if imag is None else imag + term
            out.append((real, imag))
    else:
        diff = [u[l] - u[half - l] for l in range(1, mid)]
        both = [u[l] + u[half - l] for l in range(1, mid)]
        for m in range(mid):
            k = 2 * m + 1
            real = u[0]
            imag = u[mid] * -math.sin(math.pi * k / 2)
            for l in range(1, mid):
                real = real + diff[l - 1] * math.cos(2 * math.pi * l * k / levels)
                imag = imag + both[l - 1] * -math.sin(2 * math.pi * l * k / levels)
            out.append((real, imag))
    return out


def inverse_modes(v, half, levels, odd):
    mid = half // 2
    out = [None] * half
    scale = 2.0 / levels
    for l in range(mid + 1):
        if not odd:
            cosine = v[0] * (1.0 / levels) + v[1] * ((-1.0) ** l / levels)
            sine = None
            for m in range(1, mid):
                cosine = cosine + v[2 * m] * (scale * math.cos(2 * math.pi * l * m / half))
                if l not in (0, mid):
                    term = v[2 * m + 1] * (scale * math.sin(2 * math.pi * l * m / half))
                    sine = term if sine is None else sine + term
            low = cosine if sine is None else cosine - sine
            high = cosine if sine is None else cosine + sine
        else:
            cosine = sine = None
            for m in range(mid):
                k = 2 * m + 1
                term = v[2 * m] * (scale * math.cos(2 * math.pi * l * k / levels))
                cosine = term if cosine is None else cosine + term
                if l > 0:
                    term = v[2 * m + 1] * (scale * math.sin(2 * math.pi * l * k / levels))
                    sine = term if sine is None else sine + term
            low = cosine if sine is None else cosine - sine
            high = -cosine if sine is None else -cosine - sine
        out[l] = low
        if 0 < l < half:
            out[half - l] = high if l != mid else low
    return out


def kernel(
    levels, stripes,
    guess_ref, start_ref, bed_ref, rate_ref, balance_ref, flags_ref,
    out_ref,
    guess, balance, bed_in, rate_in, flags_in,
    own, edge, mass, stat_send, stat, row_send, rows, row_dummy,
    dsend, dext, resid, ysend, yext, coef, mean_pad, weight, work, modes, parts, dummy,
    load_sem, gsend, grecv, bsend, brecv, ssend, srecv, osend, orecv,
    esend, erecv, hsend, hrecv, dsem_s, dsem_r, ysem_s, ysem_r,
    psem_s, psem_r, qsem_s, qsem_r,
):
    half = levels // 2
    slots = half // 2
    ring_z = levels // RING_Y
    tiles = stripes * levels
    root = circulant_weight ** (1.0 / levels)
    group = min(GROUP, slots)
    chunk = min(CHUNK, group)

    level = lax.axis_index("tm")
    sx = lax.axis_index("sx")
    core = lax.axis_index("sy")
    other = 1 - core

    def turned(stripe, index):
        return index ^ ((stripe & 1) * (levels - 1))

    def snake(index):
        return index ^ (((index >> 2) & 1) * (RING_Y - 1))

    def tile_of(stripe, tm):
        return turned(stripe, snake(tm))

    def owner_of(stripe, tile):
        return snake(turned(stripe, tile))

    tile = tile_of(sx, level)
    strip = sx * levels + tile
    above = (strip + tiles - 1) & (tiles - 1)
    below = (strip + 1) & (tiles - 1)
    above_sx, below_sx = lax.div(above, levels), lax.div(below, levels)
    above_tm = owner_of(above_sx, above & (levels - 1))
    below_tm = owner_of(below_sx, below & (levels - 1))
    has_above = strip > 0
    has_below = strip < tiles - 1

    def reach(code, ring):
        return -sum(min((p ^ code) - p & ring - 1, p - (p ^ code) & ring - 1) for p in range(ring))

    far_z = sorted(range(ring_z), key=lambda code: reach(code, ring_z))
    far_y = sorted(range(RING_Y), key=lambda code: reach(code, RING_Y))
    peers = [level ^ (z * RING_Y + y) for z in far_z for y in far_y if z or y]

    def send(src, dst, ssem, rsem, device):
        pltpu.make_async_remote_copy(
            src_ref=src, dst_ref=dst, send_sem=ssem, recv_sem=rsem,
            device_id=device, device_id_type=MESH,
        ).start()

    def wait(sem, count):
        view = dummy.at[pl.ds(0, count)]
        pltpu.make_async_copy(view, view, sem).wait()

    def wait_rows(sem, count):
        view = row_dummy.at[pl.ds(0, count)]
        pltpu.make_async_copy(view, view, sem).wait()

    def around(src, place, ssem, rsem):
        for to in range(2):
            send(src, place(2), ssem, rsem, (above_tm, above_sx, to))
            send(src, place(0), ssem, rsem, (below_tm, below_sx, to))
        send(src, place(1), ssem, rsem, (level, sx, other))

    barrier = pltpu.get_barrier_semaphore()

    def greet(device):
        pl.semaphore_signal(barrier, inc=1, device_id=device, device_id_type=MESH)

    for peer in peers:
        greet((peer, sx, core))
    greet((level, sx, other))
    for to in range(2):
        greet((above_tm, above_sx, to))
        greet((below_tm, below_sx, to))

    next_sx = (sx + 1) & (stripes - 1)
    prev_sx = (sx + stripes - 1) & (stripes - 1)
    at_start, at_end = tile == 0, tile == levels - 1
    for at, stripe in ((at_start, prev_sx), (at_end, next_sx)):
        @pl.when(at)
        def _():
            def tell(tm, carry):
                greet((tm, stripe, core))
                return carry

            lax.fori_loop(0, levels, tell, 0)

    here = pl.ds(pl.multiple_of(tile * ROWS, ROWS), ROWS)
    loads = [
        pltpu.make_async_copy(guess_ref.at[0], guess, load_sem.at[0]),
        pltpu.make_async_copy(balance_ref.at[0], balance, load_sem.at[1]),
        pltpu.make_async_copy(bed_ref.at[here], bed_in, load_sem.at[2]),
        pltpu.make_async_copy(rate_ref.at[here], rate_in, load_sem.at[3]),
        pltpu.make_async_copy(flags_ref.at[here], flags_in, load_sem.at[4]),
        pltpu.make_async_copy(start_ref.at[here], own.at[0, core], load_sem.at[5]),
    ]
    for load in loads:
        load.start()
    row8 = lax.broadcasted_iota(jnp.int32, (ROWS, LANES), 0)
    lane = lax.broadcasted_iota(jnp.int32, (ROWS, LANES), 1)
    first_row, last_row = row8 == 0, row8 == ROWS - 1
    first_lane, last_lane = lane == 0, lane == LANES - 1
    row24 = lax.broadcasted_iota(jnp.int32, (EXT, LANES), 0)
    lane24 = lax.broadcasted_iota(jnp.int32, (EXT, LANES), 1)
    first24, last24 = lane24 == 0, lane24 == LANES - 1
    edge_valid = (last_row & has_above) | (first_row & has_below)
    valid24 = ((row24 >= ROWS) | has_above) & ((row24 < 2 * ROWS) | has_below)
    zero = jnp.zeros((ROWS, LANES), jnp.float32)
    for h in range(2):
        for pad in (pl.ds(0, ROWS), pl.ds(ROWS + EXT, ROWS)):
            mean_pad[h, pad] = zero
            for turn in range(2):
                for slot in range(group):
                    for i in range(2):
                        work[turn, slot, i, h, pad] = zero
    for load in loads:
        load.wait()

    inside_own = (flags_in[...] != 0).astype(jnp.float32)
    boost = 1.0 + (flags_in[...] == 2).astype(jnp.float32)
    cst_own = inside_own * boost * rate_in[...]
    bed_own = bed_in[...]
    for i, value in enumerate((cst_own, bed_own, inside_own)):
        stat_send[i] = value
        stat[i, core, ROWS : 2 * ROWS] = value

    for t in range(levels):
        row_send[0, t] = guess[t * ROWS + ROWS - 1 : t * ROWS + ROWS]
        row_send[1, t] = guess[t * ROWS : t * ROWS + 1]

    pl.semaphore_wait(barrier, levels - 1 + 5 + 2)

    def scatter(src, dst, ssem, rsem):
        for peer in peers:
            rows_to = pl.ds(pl.multiple_of(tile_of(sx, peer) * ROWS, ROWS), ROWS)
            send(src.at[rows_to], dst, ssem, rsem, (peer, sx, core))

    scatter(guess, own.at[1 + level, core], gsend, grecv)
    for peer in peers:
        to = tile_of(sx, peer)

        @pl.when(to > 0)
        def _():
            send(row_send.at[0, to - 1], rows.at[0, level], esend, erecv, (peer, sx, core))

        @pl.when(to < levels - 1)
        def _():
            send(row_send.at[1, to + 1], rows.at[1, level], esend, erecv, (peer, sx, core))

    send(
        row_send.at[0, levels - 1], rows.at[0, level], esend, erecv,
        (owner_of(next_sx, 0), next_sx, core),
    )
    send(
        row_send.at[1, 0], rows.at[1, level], esend, erecv,
        (owner_of(prev_sx, levels - 1), prev_sx, core),
    )

    @pl.when(tile > 0)
    def _():
        rows[0, level] = row_send[0, tile - 1]

    @pl.when(tile < levels - 1)
    def _():
        rows[1, level] = row_send[1, tile + 1]

    scatter(balance, mass.at[level], bsend, brecv)
    around(stat_send, lambda p: stat.at[:, core, pl.ds(p * ROWS, ROWS)], ssend, srecv)
    own[1 + level, core] = guess[here]
    mass[level] = balance[here]

    wait(grecv, levels - 1)
    mine = own.at[pl.ds(1, levels), core]
    send(mine, mine, hsend, hrecv, (level, sx, other))

    def neighbours(x, x_other, x_edge):
        right = pltpu.roll(jnp.where(first_lane, jnp.where(core == 0, x_other, 0.0), x), LANES - 1, 1)
        left = pltpu.roll(jnp.where(last_lane, jnp.where(core == 1, x_other, 0.0), x), 1, 1)
        down = pltpu.roll(jnp.where(first_row, x_edge, x), ROWS - 1, 0)
        up = pltpu.roll(jnp.where(last_row, x_edge, x), 1, 0)
        return right, left, down, up

    wait(srecv, 3 * 5)

    @pl.when(at_start | at_end)
    def _():
        wait_rows(erecv, 2 * levels - 1)

    @pl.when(jnp.logical_not(at_start | at_end))
    def _():
        wait_rows(erecv, 2 * levels - 2)

    for l in range(levels):
        edge[l] = jnp.where(last_row, rows[0, l], rows[1, l])

    cst_other = stat[0, other, ROWS : 2 * ROWS]
    bed_other = stat[1, other, ROWS : 2 * ROWS]
    cst_edge = jnp.where(
        edge_valid, jnp.where(last_row, stat[0, core, 0:ROWS], stat[0, core, 2 * ROWS :]), 0.0
    )
    bed_edge = jnp.where(last_row, stat[1, core, 0:ROWS], stat[1, core, 2 * ROWS :])

    wait(hrecv, levels)

    def diffusivity(scale, h):
        return scale * h * h * jnp.abs(h)

    def newton(n, carry):
        more = n < NEWTON - 1

        sums = [zero, zero, zero]
        for l in range(levels):
            sums[0] = sums[0] + diffusivity(cst_own, own[1 + l, core])
            sums[1] = sums[1] + diffusivity(cst_other, own[1 + l, other])
            sums[2] = sums[2] + diffusivity(cst_edge, edge[l])
        mean, mean_other, mean_edge = (s * (1.0 / levels) for s in sums)
        total = 0.5 * (4.0 * mean + sum(neighbours(mean, mean_other, mean_edge)))
        for i, value in enumerate((mean, total)):
            dsend[n, i] = value
            dext[n, i, core, ROWS : 2 * ROWS] = value
        around(
            dsend.at[n], lambda p: dext.at[n, :, core, pl.ds(p * ROWS, ROWS)],
            dsem_s.at[n], dsem_r.at[n],
        )

        @pl.when(n == 0)
        def _():
            wait(brecv, levels - 1)

        for l in range(levels):
            h, h_other, h_edge = own[1 + l, core], own[1 + l, other], edge[l]
            s = h + bed_own
            d_near = neighbours(
                diffusivity(cst_own, h), diffusivity(cst_other, h_other),
                diffusivity(cst_edge, h_edge),
            )
            s_near = neighbours(
                s, h_other + bed_other, jnp.where(edge_valid, h_edge + bed_edge, 0.0)
            )
            d = diffusivity(cst_own, h)
            flux = sum((d + dn) * (s - sn) for dn, sn in zip(d_near, s_near))
            change = (h - own[l, core]) / time_step + 0.5 * flux - mass[l]
            resid[l] = inside_own * change * (root ** l)

        low = [resid[l] for l in range(half)]
        high = [resid[l + half] for l in range(half)]
        evens = forward_modes([a + b for a, b in zip(low, high)], half, levels, False)
        odds = forward_modes([a - b for a, b in zip(low, high)], half, levels, True)
        for slot in range(slots):
            for i in range(2):
                ysend[n, 0, 2 * slot + i] = evens[slot][i]
                ysend[n, 1, 2 * slot + i] = odds[slot][i]
                yext[n, 2 * slot + i, core, ROWS : 2 * ROWS] = jnp.where(
                    core == 0, evens[slot][i], odds[slot][i]
                )
            if slot % chunk != chunk - 1:
                continue
            pair = pl.ds(2 * (slot + 1 - chunk), 2 * chunk)

            def place(p):
                return yext.at[n, pair, core, pl.ds(p * ROWS, ROWS)]

            s_sem, r_sem = ysem_s.at[n], ysem_r.at[n, slot // chunk]
            for to in range(2):
                send(ysend.at[n, to, pair], place(2), s_sem, r_sem, (above_tm, above_sx, to))
                send(ysend.at[n, to, pair], place(0), s_sem, r_sem, (below_tm, below_sx, to))
            send(ysend.at[n, other, pair], place(1), s_sem, r_sem, (level, sx, other))

        wait(dsem_r.at[n], 2 * 5)
        inner = pl.ds(ROWS, EXT)
        m0, m1 = (jnp.where(valid24, dext[n, 0, h], 0.0) for h in range(2))
        mean_pad[0, inner] = m0
        mean_pad[1, inner] = m1
        weight[0, 0] = 0.5 * (m0 + pltpu.roll(jnp.where(first24, m1, m0), LANES - 1, 1))
        weight[0, 1] = jnp.where(last24, 0.0, 0.5 * (m1 + pltpu.roll(m1, LANES - 1, 1)))
        weight[1, 0] = jnp.where(first24, 0.0, 0.5 * (m0 + pltpu.roll(m0, 1, 1)))
        weight[1, 1] = 0.5 * (m1 + pltpu.roll(jnp.where(last24, m0, m1), 1, 1))
        for h, m in ((0, m0), (1, m1)):
            weight[2, h] = 0.5 * (m + mean_pad[h, pl.ds(ROWS + 1, EXT)])
            weight[3, h] = 0.5 * (m + mean_pad[h, pl.ds(ROWS - 1, EXT)])

        def shift(k):
            angle = 2 * math.pi * k / levels
            return (
                (1.0 - root * math.cos(angle)) / time_step,
                root * math.sin(angle) / time_step,
            )

        for m in range(slots):
            even_real, even_imag = shift(2 * m)
            odd_real, odd_imag = shift(2 * m + 1)
            last_real = shift(half)[0] if m == 0 else even_real
            imag = jnp.where(core == 0, 0.0 if m == 0 else even_imag, odd_imag)
            for h in range(2):
                inside = jnp.where(valid24, stat[2, h], 0.0)
                real = dext[n, 1, h] + jnp.where(core == 0, even_real, odd_real)
                scaled = inside / (real * real + imag * imag)
                coef[m, 0, h] = scaled * real
                coef[m, 1, h] = scaled * -imag
                if m == 0:
                    real = dext[n, 1, h] + jnp.where(core == 0, last_real, odd_real)
                    coef[m, 2, h] = inside * real / (real * real + imag * imag)
                else:
                    coef[m, 2, h] = scaled * real

        def solve(g, carry):
            for i in range(group // chunk):
                wait(ysem_r.at[n, g * (group // chunk) + i], 2 * 5 * chunk)

            def apply(i, h, t, real, imag):
                rows_t = slice(t * ROWS, (t + 1) * ROWS)
                a, b = (coef[g * group + i, k, h, rows_t] for k in range(2))
                c = coef[g * group, 2, h, rows_t] if i == 0 else a
                return real * a - imag * b, real * b + imag * c

            def source(i, part, h, t):
                return yext[n, 2 * (g * group + i) + part, h, t * ROWS : (t + 1) * ROWS]

            blocks = [(h, t) for h in range(2) for t in range(EXT // ROWS)]
            for i in range(group):
                for h, t in blocks:
                    value = apply(i, h, t, source(i, 0, h, t), source(i, 1, h, t))
                    for part in range(2):
                        work[0, i, part, h, pl.ds(ROWS * (1 + t), ROWS)] = value[part]
            for sweep in range(SWEEPS - 1):
                now, then = sweep % 2, (sweep + 1) % 2
                for first in range(0, group, 2):
                    pair = range(first, min(first + 2, group))
                    right, left, last = {}, {}, {}
                    for i in pair:
                        for part in range(2):
                            v0, v1 = work[now, i, part, 0, inner], work[now, i, part, 1, inner]
                            right[i, part] = (
                                pltpu.roll(jnp.where(first24, v1, v0), LANES - 1, 1),
                                pltpu.roll(v1, LANES - 1, 1),
                            )
                            left[i, part] = (
                                pltpu.roll(v0, 1, 1),
                                pltpu.roll(jnp.where(last24, v0, v1), 1, 1),
                            )
                    for h, t in blocks:
                        rows_t = slice(t * ROWS, (t + 1) * ROWS)
                        w = [weight[k, h, rows_t] for k in range(4)]
                        for i in pair:
                            total_t = [
                                source(i, part, h, t)
                                + w[0] * right[i, part][h][rows_t]
                                + w[1] * left[i, part][h][rows_t]
                                + w[2] * work[now, i, part, h, pl.ds(ROWS * (1 + t) + 1, ROWS)]
                                + w[3] * work[now, i, part, h, pl.ds(ROWS * (1 + t) - 1, ROWS)]
                                for part in range(2)
                            ]
                            value = apply(i, h, t, *total_t)
                            for part in range(2):
                                if sweep < SWEEPS - 2:
                                    work[then, i, part, h, pl.ds(ROWS * (1 + t), ROWS)] = value[part]
                                else:
                                    last[i, part, h, t] = value[part]
                    for (i, part, h, t), v in last.items():
                        field = 2 * (g * group + i) + part
                        if t == 1:
                            modes[h, field] = v
                        elif t == 2:
                            modes[2 + h, field] = jnp.where(last_row, last[i, part, h, 0], v)
            return carry

        lax.fori_loop(0, slots // group, solve, 0)

        for parity in range(2):
            @pl.when(core == parity)
            def _():
                def invert(i, carry):
                    p = (i & 2) + jnp.where((i & 1) == 0, other, core)
                    values = inverse_modes(
                        [modes[p, f] for f in range(half)], half, levels, parity == 1
                    )
                    for l in range(half):
                        parts[n, parity, p, l] = values[l]
                    block = parts.at[n, parity, p]

                    @pl.when(i == 0)
                    def _():
                        send(block, block, psem_s.at[n], psem_r.at[n], (level, sx, other))

                    @pl.when((i > 0) & (i < 3) & more)
                    def _():
                        send(block, block, qsem_s, qsem_r, (level, sx, other))

                    return carry

                lax.fori_loop(0, jnp.where(more, 4, 2), invert, 0)

        @pl.when(n == 0)
        def _():
            wait(hsend, levels)

        def update(target, p):
            for l in range(half):
                drop = root ** -l
                even, odd = parts[n, 0, p, l], parts[n, 1, p, l]
                near, far = target(l), target(l + half)
                near[...] = near[...] - (even + odd) * drop
                far[...] = far[...] - (even - odd) * (drop * root ** -half)

        wait(psem_r.at[n], half)
        update(lambda l: own.at[1 + l, core], core)

        @pl.when(more)
        def _():
            wait(qsem_r, 2 * half)
            update(lambda l: own.at[1 + l, other], other)
            update(lambda l: edge.at[l], 2 + core)

        return carry

    lax.fori_loop(0, NEWTON, newton, 0)

    for peer in peers:
        send(own.at[1 + peer, core], out_ref.at[0, here], osend, orecv, (peer, sx, core))
    out_ref[0, here] = own[1 + level, core]

    wait(gsend, levels - 1)
    wait(bsend, levels - 1)
    wait(ssend, 3 * 5)

    @pl.when(at_start | at_end)
    def _():
        wait_rows(esend, 2 * levels - 1)

    @pl.when(jnp.logical_not(at_start | at_end))
    def _():
        wait_rows(esend, 2 * levels - 2)

    for n in range(NEWTON):
        wait(dsem_s.at[n], 2 * 5)
        wait(ysem_s.at[n], 2 * 5 * slots)
        wait(psem_s.at[n], half)
    if NEWTON > 1:
        wait(qsem_s, 2 * half * (NEWTON - 1))
    wait(osend, levels - 1)
    wait(orecv, levels - 1)


def solution(mesh):
    levels, stripes = mesh.shape["tm"], mesh.shape["sx"]
    half = levels // 2
    slots = half // 2
    tile = (ROWS, LANES)
    wide = (EXT, LANES)
    padded = (EXT + 2 * ROWS, LANES)
    f32 = jnp.float32

    def vmem(*lead, last=tile, dtype=f32):
        return pltpu.VMEM((*lead, *last), dtype)

    dma = pltpu.SemaphoreType.DMA

    def body(guess, start, bed, rate, balance, flags):
        rows = guess.shape[1]
        return pl.pallas_call(
            functools.partial(kernel, levels, stripes),
            out_shape=pltpu.VMEM(guess.shape, f32),
            in_specs=[pl.BlockSpec(memory_space=pl.ANY)] * 6,
            out_specs=pl.BlockSpec(memory_space=pltpu.VMEM),
            scratch_shapes=[
                vmem(last=(rows, LANES)), vmem(last=(rows, LANES)),
                vmem(), vmem(), vmem(dtype=jnp.int32),
                vmem(levels + 1, 2), vmem(levels), vmem(levels),
                vmem(3), vmem(3, 2, last=wide),
                vmem(2, levels, last=(1, LANES)), vmem(2, levels, last=(1, LANES)),
                vmem(2 * levels, last=(1, LANES)),
                vmem(NEWTON, 2), vmem(NEWTON, 2, 2, last=wide),
                vmem(levels), vmem(NEWTON, 2, half),
                vmem(NEWTON, half, 2, last=wide),
                vmem(slots, 3, 2, last=wide), vmem(2, last=padded), vmem(4, 2, last=wide),
                vmem(2, min(GROUP, slots), 2, 2, last=padded),
                vmem(4, half), vmem(NEWTON, 2, 4, half),
                vmem(max(2 * 5 * slots, 4 * half, levels)),
                dma((6,)), dma, dma, dma, dma, dma, dma, dma, dma,
                dma, dma, dma, dma, dma((NEWTON,)), dma((NEWTON,)),
                dma((NEWTON,)), dma((NEWTON, slots)), dma((NEWTON,)), dma((NEWTON,)), dma, dma,
            ],
            compiler_params=pltpu.CompilerParams(collective_id=0, has_side_effects=True),
        )(guess, start, bed, rate, balance, flags)

    return jax.shard_map(
        body, mesh=mesh,
        in_specs=(
            P("tm", "sx", "sy"), P("sx", "sy"), P("sx", "sy"), P("sx", "sy"),
            P("tm", "sx", "sy"), P("sx", "sy"),
        ),
        out_specs=P("tm", "sx", "sy"), check_vma=False,
    )
```

```python
import functools
import math

import jax
import jax.numpy as jnp
from jax import lax
from jax.experimental import pallas as pl
from jax.experimental.pallas import tpu as pltpu
from jax.sharding import PartitionSpec as P

NEWTON = 2
SWEEPS = 8
RING_Y = 4
ROWS = 8
LANES = 128
EXT = 3 * ROWS
GROUPS = (4, 4)

circulant_weight = 0.25
time_step = 1.0
MESH = pl.DeviceIdType.MESH


def forward_modes(u, half, levels, odd):
    mid = half // 2
    out = []
    if not odd:
        even = [u[l] + u[half - l] for l in range(1, mid)]
        diff = [u[l] - u[half - l] for l in range(1, mid)]
        plus, minus = u[0] + u[mid], u[0] - u[mid]
        for m in range(mid):
            real = plus if m % 2 == 0 else minus
            for l in range(1, mid):
                real = real + even[l - 1] * math.cos(2 * math.pi * l * m / half)
            if m == 0:
                imag = plus if mid % 2 == 0 else minus
                for l in range(1, mid):
                    imag = imag + even[l - 1] * (-1.0) ** l
            else:
                imag = None
                for l in range(1, mid):
                    term = diff[l - 1] * -math.sin(2 * math.pi * l * m / half)
                    imag = term if imag is None else imag + term
            out.append((real, imag))
    else:
        diff = [u[l] - u[half - l] for l in range(1, mid)]
        both = [u[l] + u[half - l] for l in range(1, mid)]
        for m in range(mid):
            k = 2 * m + 1
            real = u[0]
            imag = u[mid] * -math.sin(math.pi * k / 2)
            for l in range(1, mid):
                real = real + diff[l - 1] * math.cos(2 * math.pi * l * k / levels)
                imag = imag + both[l - 1] * -math.sin(2 * math.pi * l * k / levels)
            out.append((real, imag))
    return out


def inverse_modes(v, half, levels, odd):
    mid = half // 2
    out = [None] * half
    scale = 2.0 / levels
    for l in range(mid + 1):
        if not odd:
            cosine = v[0] * (1.0 / levels) + v[1] * ((-1.0) ** l / levels)
            sine = None
            for m in range(1, mid):
                cosine = cosine + v[2 * m] * (scale * math.cos(2 * math.pi * l * m / half))
                if l not in (0, mid):
                    term = v[2 * m + 1] * (scale * math.sin(2 * math.pi * l * m / half))
                    sine = term if sine is None else sine + term
            low = cosine if sine is None else cosine - sine
            high = cosine if sine is None else cosine + sine
        else:
            cosine = sine = None
            for m in range(mid):
                k = 2 * m + 1
                term = v[2 * m] * (scale * math.cos(2 * math.pi * l * k / levels))
                cosine = term if cosine is None else cosine + term
                if l > 0:
                    term = v[2 * m + 1] * (scale * math.sin(2 * math.pi * l * k / levels))
                    sine = term if sine is None else sine + term
            low = cosine if sine is None else cosine - sine
            high = -cosine if sine is None else -cosine - sine
        out[l] = low
        if 0 < l < half:
            out[half - l] = high if l != mid else low
    return out


def kernel(
    levels, stripes,
    guess_ref, start_ref, bed_ref, rate_ref, balance_ref, flags_ref,
    out_ref,
    guess, balance, bed_in, rate_in, flags_in,
    own, edge, mass, stat_send, stat, row_send, rows, rows_far, row_dummy,
    dsend, dext, resid, ysend, yext, coef, mean_pad, weight, work, modes, parts, dummy,
    load_sem, gsend, grecv, bsend, brecv, ssend, srecv, osend, orecv,
    esend, erecv, frecv, hsend, hrecv, dsem_s, dsem_r, ysem_s, ysem_r,
    psem_s, psem_r, qsem_s, qsem_r,
):
    half = levels // 2
    slots = half // 2
    ring_z = levels // RING_Y
    tiles = stripes * levels
    root = circulant_weight ** (1.0 / levels)
    groups = GROUPS if sum(GROUPS) == slots else (slots,)
    starts = [sum(groups[:i]) for i in range(len(groups))]
    most = max(groups)

    level = lax.axis_index("tm")
    sx = lax.axis_index("sx")
    core = lax.axis_index("sy")
    other = 1 - core

    def turned(stripe, index):
        return index ^ ((stripe & 1) * (levels - 1))

    def snake(index):
        return index ^ (((index >> 2) & 1) * (RING_Y - 1))

    def tile_of(stripe, tm):
        return turned(stripe, snake(tm))

    def owner_of(stripe, tile):
        return snake(turned(stripe, tile))

    tile = tile_of(sx, level)
    strip = sx * levels + tile
    above = (strip + tiles - 1) & (tiles - 1)
    below = (strip + 1) & (tiles - 1)
    above_sx, below_sx = lax.div(above, levels), lax.div(below, levels)
    above_tm = owner_of(above_sx, above & (levels - 1))
    below_tm = owner_of(below_sx, below & (levels - 1))
    has_above = strip > 0
    has_below = strip < tiles - 1

    def reach(code, ring):
        return -sum(min((p ^ code) - p & ring - 1, p - (p ^ code) & ring - 1) for p in range(ring))

    far_z = sorted(range(ring_z), key=lambda code: reach(code, ring_z))
    far_y = sorted(range(RING_Y), key=lambda code: reach(code, RING_Y))
    peers = [level ^ (z * RING_Y + y) for z in far_z for y in far_y if z or y]

    def send(src, dst, ssem, rsem, device):
        pltpu.make_async_remote_copy(
            src_ref=src, dst_ref=dst, send_sem=ssem, recv_sem=rsem,
            device_id=device, device_id_type=MESH,
        ).start()

    def wait(sem, count):
        view = dummy.at[pl.ds(0, count)]
        pltpu.make_async_copy(view, view, sem).wait()

    def wait_rows(sem, count):
        view = row_dummy.at[pl.ds(0, count)]
        pltpu.make_async_copy(view, view, sem).wait()

    def around(src, place, ssem, rsem):
        for to in range(2):
            send(src, place(2), ssem, rsem, (above_tm, above_sx, to))
            send(src, place(0), ssem, rsem, (below_tm, below_sx, to))
        send(src, place(1), ssem, rsem, (level, sx, other))

    barrier = pltpu.get_barrier_semaphore()

    def greet(device):
        pl.semaphore_signal(barrier, inc=1, device_id=device, device_id_type=MESH)

    for peer in peers:
        greet((peer, sx, core))
    greet((level, sx, other))
    for to in range(2):
        greet((above_tm, above_sx, to))
        greet((below_tm, below_sx, to))

    next_sx = (sx + 1) & (stripes - 1)
    prev_sx = (sx + stripes - 1) & (stripes - 1)
    at_start, at_end = tile == 0, tile == levels - 1
    for at, stripe in ((at_start, prev_sx), (at_end, next_sx)):
        @pl.when(at)
        def _():
            def tell(tm, carry):
                greet((tm, stripe, core))
                return carry

            lax.fori_loop(0, levels, tell, 0)

    here = pl.ds(pl.multiple_of(tile * ROWS, ROWS), ROWS)
    loads = [
        pltpu.make_async_copy(guess_ref.at[0], guess, load_sem.at[0]),
        pltpu.make_async_copy(balance_ref.at[0], balance, load_sem.at[1]),
        pltpu.make_async_copy(bed_ref.at[here], bed_in, load_sem.at[2]),
        pltpu.make_async_copy(rate_ref.at[here], rate_in, load_sem.at[3]),
        pltpu.make_async_copy(flags_ref.at[here], flags_in, load_sem.at[4]),
        pltpu.make_async_copy(start_ref.at[here], own.at[0, core], load_sem.at[5]),
    ]
    for load in loads:
        load.start()
    row8 = lax.broadcasted_iota(jnp.int32, (ROWS, LANES), 0)
    lane = lax.broadcasted_iota(jnp.int32, (ROWS, LANES), 1)
    first_row, last_row = row8 == 0, row8 == ROWS - 1
    first_lane, last_lane = lane == 0, lane == LANES - 1
    row24 = lax.broadcasted_iota(jnp.int32, (EXT, LANES), 0)
    lane24 = lax.broadcasted_iota(jnp.int32, (EXT, LANES), 1)
    first24, last24 = lane24 == 0, lane24 == LANES - 1
    edge_valid = (last_row & has_above) | (first_row & has_below)
    valid24 = ((row24 >= ROWS) | has_above) & ((row24 < 2 * ROWS) | has_below)
    zero = jnp.zeros((ROWS, LANES), jnp.float32)
    for h in range(2):
        for pad in (pl.ds(0, ROWS), pl.ds(ROWS + EXT, ROWS)):
            mean_pad[h, pad] = zero
            for turn in range(2):
                for slot in range(most):
                    for i in range(2):
                        work[turn, slot, i, h, pad] = zero
    for load in loads:
        load.wait()

    inside_own = (flags_in[...] != 0).astype(jnp.float32)
    boost = 1.0 + (flags_in[...] == 2).astype(jnp.float32)
    cst_own = inside_own * boost * rate_in[...]
    bed_own = bed_in[...]
    for i, value in enumerate((cst_own, bed_own, inside_own)):
        stat_send[i] = value
        stat[i, core, ROWS : 2 * ROWS] = value

    for t in range(levels):
        for i, row in enumerate((t * ROWS - 1, t * ROWS + ROWS)):
            row = row % (levels * ROWS)
            row_send[t, i] = guess[row : row + 1]

    pl.semaphore_wait(barrier, levels - 1 + 5 + 2)

    def scatter(src, dst, ssem, rsem):
        for peer in peers:
            rows_to = pl.ds(pl.multiple_of(tile_of(sx, peer) * ROWS, ROWS), ROWS)
            send(src.at[rows_to], dst, ssem, rsem, (peer, sx, core))

    scatter(guess, own.at[1 + level, core], gsend, grecv)
    for peer in peers:
        send(row_send.at[tile_of(sx, peer)], rows.at[level], esend, erecv, (peer, sx, core))
    send(
        row_send.at[0, 0], rows_far.at[level], esend, frecv,
        (owner_of(next_sx, 0), next_sx, core),
    )
    send(
        row_send.at[levels - 1, 1], rows_far.at[level], esend, frecv,
        (owner_of(prev_sx, levels - 1), prev_sx, core),
    )
    rows[level] = row_send[tile]

    scatter(balance, mass.at[level], bsend, brecv)
    around(stat_send, lambda p: stat.at[:, core, pl.ds(p * ROWS, ROWS)], ssend, srecv)
    own[1 + level, core] = guess[here]
    mass[level] = balance[here]

    wait(grecv, levels - 1)
    mine = own.at[pl.ds(1, levels), core]
    send(mine, mine, hsend, hrecv, (level, sx, other))

    def neighbours(x, x_other, x_edge):
        right = pltpu.roll(jnp.where(first_lane, jnp.where(core == 0, x_other, 0.0), x), LANES - 1, 1)
        left = pltpu.roll(jnp.where(last_lane, jnp.where(core == 1, x_other, 0.0), x), 1, 1)
        down = pltpu.roll(jnp.where(first_row, x_edge, x), ROWS - 1, 0)
        up = pltpu.roll(jnp.where(last_row, x_edge, x), 1, 0)
        return right, left, down, up

    wait(srecv, 3 * 5)
    wait_rows(erecv, 2 * (levels - 1))
    for i, at in enumerate((at_start, at_end)):
        @pl.when(at)
        def _():
            wait_rows(frecv, levels)
            for l in range(levels):
                rows[l, i] = rows_far[l]

    for l in range(levels):
        edge[l] = jnp.where(last_row, rows[l, 0], rows[l, 1])

    cst_other = stat[0, other, ROWS : 2 * ROWS]
    bed_other = stat[1, other, ROWS : 2 * ROWS]
    cst_edge = jnp.where(
        edge_valid, jnp.where(last_row, stat[0, core, 0:ROWS], stat[0, core, 2 * ROWS :]), 0.0
    )
    bed_edge = jnp.where(last_row, stat[1, core, 0:ROWS], stat[1, core, 2 * ROWS :])

    wait(hrecv, levels)

    def diffusivity(scale, h):
        return scale * h * h * jnp.abs(h)

    def newton(n, carry):
        more = n < NEWTON - 1

        sums = [zero, zero, zero]
        for l in range(levels):
            sums[0] = sums[0] + diffusivity(cst_own, own[1 + l, core])
            sums[1] = sums[1] + diffusivity(cst_other, own[1 + l, other])
            sums[2] = sums[2] + diffusivity(cst_edge, edge[l])
        mean, mean_other, mean_edge = (s * (1.0 / levels) for s in sums)
        total = 0.5 * (4.0 * mean + sum(neighbours(mean, mean_other, mean_edge)))
        for i, value in enumerate((mean, total)):
            dsend[n, i] = value
            dext[n, i, core, ROWS : 2 * ROWS] = value
        around(
            dsend.at[n], lambda p: dext.at[n, :, core, pl.ds(p * ROWS, ROWS)],
            dsem_s.at[n], dsem_r.at[n],
        )

        @pl.when(n == 0)
        def _():
            wait(brecv, levels - 1)

        for l in range(levels):
            h, h_other, h_edge = own[1 + l, core], own[1 + l, other], edge[l]
            s = h + bed_own
            d_near = neighbours(
                diffusivity(cst_own, h), diffusivity(cst_other, h_other),
                diffusivity(cst_edge, h_edge),
            )
            s_near = neighbours(
                s, h_other + bed_other, jnp.where(edge_valid, h_edge + bed_edge, 0.0)
            )
            d = diffusivity(cst_own, h)
            flux = sum((d + dn) * (s - sn) for dn, sn in zip(d_near, s_near))
            change = (h - own[l, core]) / time_step + 0.5 * flux - mass[l]
            resid[l] = inside_own * change * (root ** l)

        low = [resid[l] for l in range(half)]
        high = [resid[l + half] for l in range(half)]
        evens = forward_modes([a + b for a, b in zip(low, high)], half, levels, False)
        odds = forward_modes([a - b for a, b in zip(low, high)], half, levels, True)
        for slot in range(slots):
            for i in range(2):
                ysend[n, 0, 2 * slot + i] = evens[slot][i]
                ysend[n, 1, 2 * slot + i] = odds[slot][i]
                yext[n, 2 * slot + i, core, ROWS : 2 * ROWS] = jnp.where(
                    core == 0, evens[slot][i], odds[slot][i]
                )
            if slot + 1 not in starts[1:] + [slots]:
                continue
            index = max(i for i, start in enumerate(starts) if start <= slot)
            pair = pl.ds(2 * starts[index], 2 * groups[index])

            def place(p):
                return yext.at[n, pair, core, pl.ds(p * ROWS, ROWS)]

            s_sem, r_sem = ysem_s.at[n], ysem_r.at[n, index]
            for to in range(2):
                send(ysend.at[n, to, pair], place(2), s_sem, r_sem, (above_tm, above_sx, to))
                send(ysend.at[n, to, pair], place(0), s_sem, r_sem, (below_tm, below_sx, to))
            send(ysend.at[n, other, pair], place(1), s_sem, r_sem, (level, sx, other))

        wait(dsem_r.at[n], 2 * 5)
        inner = pl.ds(ROWS, EXT)
        m0, m1 = (jnp.where(valid24, dext[n, 0, h], 0.0) for h in range(2))
        mean_pad[0, inner] = m0
        mean_pad[1, inner] = m1
        weight[0, 0] = 0.5 * (m0 + pltpu.roll(jnp.where(first24, m1, m0), LANES - 1, 1))
        weight[0, 1] = jnp.where(last24, 0.0, 0.5 * (m1 + pltpu.roll(m1, LANES - 1, 1)))
        weight[1, 0] = jnp.where(first24, 0.0, 0.5 * (m0 + pltpu.roll(m0, 1, 1)))
        weight[1, 1] = 0.5 * (m1 + pltpu.roll(jnp.where(last24, m0, m1), 1, 1))
        for h, m in ((0, m0), (1, m1)):
            weight[2, h] = 0.5 * (m + mean_pad[h, pl.ds(ROWS + 1, EXT)])
            weight[3, h] = 0.5 * (m + mean_pad[h, pl.ds(ROWS - 1, EXT)])

        def shift(k):
            angle = 2 * math.pi * k / levels
            return (
                (1.0 - root * math.cos(angle)) / time_step,
                root * math.sin(angle) / time_step,
            )

        for m in range(slots):
            even_real, even_imag = shift(2 * m)
            odd_real, odd_imag = shift(2 * m + 1)
            last_real = shift(half)[0] if m == 0 else even_real
            imag = jnp.where(core == 0, 0.0 if m == 0 else even_imag, odd_imag)
            for h in range(2):
                inside = jnp.where(valid24, stat[2, h], 0.0)
                real = dext[n, 1, h] + jnp.where(core == 0, even_real, odd_real)
                scaled = inside / (real * real + imag * imag)
                coef[m, 0, h] = scaled * real
                coef[m, 1, h] = scaled * -imag
                if m == 0:
                    real = dext[n, 1, h] + jnp.where(core == 0, last_real, odd_real)
                    coef[m, 2, h] = inside * real / (real * real + imag * imag)
                else:
                    coef[m, 2, h] = scaled * real

        for index, (start, group) in enumerate(zip(starts, groups)):
            wait(ysem_r.at[n, index], 2 * 5 * group)

            def apply(i, h, row, real, imag):
                a, b = (coef[start + i, k, h, pl.ds(row, ROWS)] for k in range(2))
                c = coef[0, 2, h, pl.ds(row, ROWS)] if start + i == 0 else a
                return real * a - imag * b, real * b + imag * c

            def source(i, part, h, row):
                return yext[n, 2 * (start + i) + part, h, pl.ds(row, ROWS)]

            for i in range(group):
                for h in range(2):
                    for row in range(0, EXT, ROWS):
                        value = apply(i, h, row, source(i, 0, h, row), source(i, 1, h, row))
                        for part in range(2):
                            work[0, i, part, h, pl.ds(ROWS + row, ROWS)] = value[part]
            for sweep in range(SWEEPS - 1):
                now, then = sweep % 2, (sweep + 1) % 2
                base = ROWS // 2 if sweep + 1 >= ROWS // 2 else 0
                span = EXT - 2 * base
                window = pl.ds(ROWS + base, span)
                for first in range(0, group, 2):
                    pair = range(first, min(first + 2, group))
                    right, left = {}, {}
                    for i in pair:
                        for part in range(2):
                            v0, v1 = work[now, i, part, 0, window], work[now, i, part, 1, window]
                            right[i, part] = (
                                pltpu.roll(jnp.where(first24[:span], v1, v0), LANES - 1, 1),
                                pltpu.roll(v1, LANES - 1, 1),
                            )
                            left[i, part] = (
                                pltpu.roll(v0, 1, 1),
                                pltpu.roll(jnp.where(last24[:span], v0, v1), 1, 1),
                            )
                    for h in range(2):
                        for t in range(span // ROWS):
                            row = base + t * ROWS
                            rows_t = slice(t * ROWS, (t + 1) * ROWS)
                            w = [weight[k, h, pl.ds(row, ROWS)] for k in range(4)]
                            for i in pair:
                                total_t = [
                                    source(i, part, h, row)
                                    + w[0] * right[i, part][h][rows_t]
                                    + w[1] * left[i, part][h][rows_t]
                                    + w[2] * work[now, i, part, h, pl.ds(ROWS + row + 1, ROWS)]
                                    + w[3] * work[now, i, part, h, pl.ds(ROWS + row - 1, ROWS)]
                                    for part in range(2)
                                ]
                                value = apply(i, h, row, *total_t)
                                for part in range(2):
                                    work[then, i, part, h, pl.ds(ROWS + row, ROWS)] = value[part]
            final = (SWEEPS - 1) % 2
            for i in range(group):
                for part in range(2):
                    for h in range(2):
                        field = 2 * (start + i) + part
                        modes[h, field] = work[final, i, part, h, pl.ds(2 * ROWS, ROWS)]
                        modes[2 + h, field] = jnp.where(
                            last_row,
                            work[final, i, part, h, pl.ds(ROWS, ROWS)],
                            work[final, i, part, h, pl.ds(3 * ROWS, ROWS)],
                        )

        for parity in range(2):
            @pl.when(core == parity)
            def _():
                def invert(i, carry):
                    p = (i & 2) + jnp.where((i & 1) == 0, other, core)
                    values = inverse_modes(
                        [modes[p, f] for f in range(half)], half, levels, parity == 1
                    )
                    for l in range(half):
                        parts[n, parity, p, l] = values[l]
                    block = parts.at[n, parity, p]

                    @pl.when(i == 0)
                    def _():
                        send(block, block, psem_s.at[n], psem_r.at[n], (level, sx, other))

                    @pl.when((i > 0) & (i < 3) & more)
                    def _():
                        send(block, block, qsem_s, qsem_r, (level, sx, other))

                    return carry

                lax.fori_loop(0, jnp.where(more, 4, 2), invert, 0)

        @pl.when(n == 0)
        def _():
            wait(hsend, levels)

        def update(target, p):
            for l in range(half):
                drop = root ** -l
                even, odd = parts[n, 0, p, l], parts[n, 1, p, l]
                near, far = target(l), target(l + half)
                near[...] = near[...] - (even + odd) * drop
                far[...] = far[...] - (even - odd) * (drop * root ** -half)

        wait(psem_r.at[n], half)
        update(lambda l: own.at[1 + l, core], core)

        @pl.when(more)
        def _():
            wait(qsem_r, 2 * half)
            update(lambda l: own.at[1 + l, other], other)
            update(lambda l: edge.at[l], 2 + core)

        return carry

    lax.fori_loop(0, NEWTON, newton, 0)

    for peer in peers:
        send(own.at[1 + peer, core], out_ref.at[0, here], osend, orecv, (peer, sx, core))
    out_ref[0, here] = own[1 + level, core]

    wait(gsend, levels - 1)
    wait(bsend, levels - 1)
    wait(ssend, 3 * 5)
    wait_rows(esend, 2 * levels)
    for n in range(NEWTON):
        wait(dsem_s.at[n], 2 * 5)
        wait(ysem_s.at[n], 2 * 5 * slots)
        wait(psem_s.at[n], half)
    if NEWTON > 1:
        wait(qsem_s, 2 * half * (NEWTON - 1))
    wait(osend, levels - 1)
    wait(orecv, levels - 1)


def solution(mesh):
    levels, stripes = mesh.shape["tm"], mesh.shape["sx"]
    half = levels // 2
    slots = half // 2
    tile = (ROWS, LANES)
    wide = (EXT, LANES)
    padded = (EXT + 2 * ROWS, LANES)
    f32 = jnp.float32

    def vmem(*lead, last=tile, dtype=f32):
        return pltpu.VMEM((*lead, *last), dtype)

    dma = pltpu.SemaphoreType.DMA

    def body(guess, start, bed, rate, balance, flags):
        rows = guess.shape[1]
        return pl.pallas_call(
            functools.partial(kernel, levels, stripes),
            out_shape=pltpu.VMEM(guess.shape, f32),
            in_specs=[pl.BlockSpec(memory_space=pl.ANY)] * 6,
            out_specs=pl.BlockSpec(memory_space=pltpu.VMEM),
            scratch_shapes=[
                vmem(last=(rows, LANES)), vmem(last=(rows, LANES)),
                vmem(), vmem(), vmem(dtype=jnp.int32),
                vmem(levels + 1, 2), vmem(levels), vmem(levels),
                vmem(3), vmem(3, 2, last=wide),
                vmem(levels, 2, last=(1, LANES)), vmem(levels, 2, last=(1, LANES)),
                vmem(levels, last=(1, LANES)),
                vmem(2 * levels, last=(1, LANES)),
                vmem(NEWTON, 2), vmem(NEWTON, 2, 2, last=wide),
                vmem(levels), vmem(NEWTON, 2, half),
                vmem(NEWTON, half, 2, last=wide),
                vmem(slots, 3, 2, last=wide), vmem(2, last=padded), vmem(4, 2, last=wide),
                vmem(2, slots, 2, 2, last=padded),
                vmem(4, half), vmem(NEWTON, 2, 4, half),
                vmem(max(2 * 5 * slots, 4 * half, levels)),
                dma((6,)), dma, dma, dma, dma, dma, dma, dma, dma, dma,
                dma, dma, dma, dma, dma((NEWTON,)), dma((NEWTON,)),
                dma((NEWTON,)), dma((NEWTON, slots)), dma((NEWTON,)), dma((NEWTON,)), dma, dma,
            ],
            compiler_params=pltpu.CompilerParams(collective_id=0, has_side_effects=True),
        )(guess, start, bed, rate, balance, flags)

    return jax.shard_map(
        body, mesh=mesh,
        in_specs=(
            P("tm", "sx", "sy"), P("sx", "sy"), P("sx", "sy"), P("sx", "sy"),
            P("tm", "sx", "sy"), P("sx", "sy"),
        ),
        out_specs=P("tm", "sx", "sy"), check_vma=False,
    )
```
